32 devices in a mesh: gx: 8 (over y, x, core), gy: 4 (over z).
Axes of the slice: x: 2, y: 2, z: 4, core: 2. Of those that a mesh axis runs over, the one named last changes fastest.
Arguments:
- cost: float32 [16, 1024, 512], P(None, 'gx', 'gy'), may hold values from 0 to 7.5
- density_start: float32 [16, 1024, 512], P(None, 'gx', 'gy'), may hold values from 0.125 to 4.5
- coupling: float32 [16, 16], replicated, may hold values from 0 to 0.25
Outputs:
- value: float32 [16, 1024, 512], P(None, 'gx', 'gy')
- density: float32 [16, 1024, 512], P(None, 'gx', 'gy')
- ergodic: float32 [16], replicated
The draws below stay inside these ranges and needn't reach their ends.
All inputs are finite; a program needn't handle non-finite values.
Results may differ from the reference program's by a relative error of at most 0.0003.
Values sent between devices are 32-bit elements; how exact they have to be, the bound alone decides.
A program may use at most 64 MiB of HBM per device.

```python
import jax
import jax.numpy as jnp
from jax import lax

K = 16
PICARD = 1
SWEEPS = 5
NX = 1024
NY = 512


def draw_cost(key, part):
    rows = jnp.arange(NX, dtype=jnp.float32) / NX
    cols = jnp.arange(NY, dtype=jnp.float32) / NY
    ramp = 0.5 + rows[:, None] + cols[None, :]
    base = jax.random.uniform(key, (K, NX, NY), jnp.float32, 0.0, 2.0)
    return base * ramp[None]


def draw_density_start(key, part):
    rows = jnp.arange(NX, dtype=jnp.float32) / NX
    cols = jnp.arange(NY, dtype=jnp.float32) / NY
    ramp = (0.5 + rows[:, None]) * (0.5 + cols[None, :])
    base = jax.random.uniform(key, (K, NX, NY), jnp.float32, 0.5, 2.0)
    return base * ramp[None]


def setup_inputs(seed: int = 0) -> dict:
    arg_keys = jax.random.split(jax.random.key(seed), 4)
    cost = draw_cost(jax.random.fold_in(arg_keys[3], 71), 0)
    density_start = draw_density_start(jax.random.fold_in(arg_keys[3], 71), 0)
    coupling = jnp.clip(jax.random.uniform(arg_keys[2], (K, K), jnp.float32, 0.0, 0.25), 0.0, 0.25)
    return dict(cost=cost, density_start=density_start, coupling=coupling)


viscosity = 0.5
theta = 2.0


def rates(u):
    u_xp = jnp.roll(u, -1, axis=0)
    u_xm = jnp.roll(u, 1, axis=0)
    u_yp = jnp.roll(u, -1, axis=1)
    u_ym = jnp.roll(u, 1, axis=1)
    vx = -(u_xp - u_xm) * 0.5
    vy = -(u_yp - u_ym) * 0.5
    r_xp = viscosity + jnp.maximum(vx, 0.0)
    r_xm = viscosity + jnp.maximum(-vx, 0.0)
    r_yp = viscosity + jnp.maximum(vy, 0.0)
    r_ym = viscosity + jnp.maximum(-vy, 0.0)
    total = r_xp + r_xm + r_yp + r_ym
    speed = (vx * vx + vy * vy) * 0.5
    return (r_xp, r_xm, r_yp, r_ym), (u_xp, u_xm, u_yp, u_ym), total, speed


def one_class(items):
    source, value, density, lam = items
    for sweep in range(SWEEPS):
        (r_xp, r_xm, r_yp, r_ym), (u_xp, u_xm, u_yp, u_ym), total, speed = rates(value)
        trial = (source + speed - lam + r_xp * u_xp + r_xm * u_xm + r_yp * u_yp + r_ym * u_ym) / total
        shift = jnp.mean(trial)
        lam = lam + theta * shift
        value = trial - shift
    (r_xp, r_xm, r_yp, r_ym), unused, total, speed = rates(value)
    c_xp = jnp.roll(r_xm, -1, axis=0) / total
    c_xm = jnp.roll(r_xp, 1, axis=0) / total
    c_yp = jnp.roll(r_ym, -1, axis=1) / total
    c_ym = jnp.roll(r_yp, 1, axis=1) / total
    for sweep in range(SWEEPS):
        fresh = (c_xp * jnp.roll(density, -1, axis=0) + c_xm * jnp.roll(density, 1, axis=0)
                 + c_yp * jnp.roll(density, -1, axis=1) + c_ym * jnp.roll(density, 1, axis=1))
        density = fresh / jnp.mean(fresh)
    return value, density, lam


def reference(cost, density_start, coupling):
    value = jnp.zeros(cost.shape, jnp.float32)
    density = density_start
    ergodic = jnp.zeros((cost.shape[0],), jnp.float32)
    for picard in range(PICARD):
        source = cost + jnp.einsum("kj,jxy->kxy", coupling, density, precision=lax.Precision.HIGHEST)
        value, density, ergodic = lax.map(one_class, (source, value, density, ergodic))
    return value, density, ergodic
```

```python
import functools

import jax
import jax.numpy as jnp
from jax import lax
from jax.experimental import pallas as pl
from jax.experimental.pallas import tpu as pltpu
from jax.sharding import PartitionSpec as P

MESH = pl.DeviceIdType.MESH
SWEEPS = 5
THETA = 2.0
PAD = 8
CHUNK = 32
SUB = 8
GROUP = 4


def kernel(
    nx, ny,
    cost_hbm, dens_hbm, coupling,
    trial, fresh, means,
    src, u, a, b, d, cxp, cxm, cyp, cym,
    xs, xr, ps, pr, xs2, xr2, ps2, pr2,
    ar_out, ar_in, lam_tab,
    in_sem, hs_sem, hr_sem, as_sem, ar_sem,
):
    classes, rows, cols = cost_hbm.shape
    groups = classes // GROUP
    n = nx * ny
    cells = float(n * rows * cols)
    gx, gy = lax.axis_index("gx"), lax.axis_index("gy")
    up, down = lax.rem(gx + nx - 1, nx), lax.rem(gx + 1, nx)
    left, right = lax.rem(gy + ny - 1, ny), lax.rem(gy + 1, ny)
    me = gx * ny + gy

    def at(x, y):
        return {"gx": x, "gy": y}

    def each_peer(body):
        def step(i, carry):
            dx, dy = i // ny, lax.rem(i, ny)
            body(at(lax.rem(gx + dx, nx), lax.rem(gy + dy, ny)))
            return carry

        lax.fori_loop(1, n, step, 0, unroll=n - 1 if n <= 32 else 1)

    load_d = pltpu.make_async_copy(dens_hbm, d.at[0, :, pl.ds(PAD, rows), :], in_sem.at[0])
    load_c = pltpu.make_async_copy(cost_hbm, src, in_sem.at[1])
    load_d.start()
    load_c.start()

    barrier = pltpu.get_barrier_semaphore()
    each_peer(lambda dev: pl.semaphore_signal(barrier, inc=1, device_id=dev, device_id_type=MESH))

    lane = lax.broadcasted_iota(jnp.int32, (SUB, cols), 1)
    sub = lax.broadcasted_iota(jnp.int32, (SUB, cols), 0)
    lane_c = lax.broadcasted_iota(jnp.int32, (CHUNK, cols), 1)
    pair = {w: lane // (2 * w) for w in (1, 2)}

    def geometry(w):
        span = 2 * w * GROUP
        return span, rows // (cols // span)

    def pack(accs, t, k, r0, w):
        span, block = geometry(w)
        accs = list(accs)
        for i in range(CHUNK // SUB):
            r = r0 + SUB * i
            p = span * (r // block) + 2 * w * k
            q = (r % block) // SUB
            turned = pltpu.roll(t[SUB * i:SUB * i + SUB], (p + w) % cols, 1)
            accs[q] = jnp.where(pair[w] == p // (2 * w), turned, accs[q])
        return accs

    def unpack(ed, k, r0, w):
        span, block = geometry(w)
        parts = []
        for i in range(CHUNK // SUB):
            r = r0 + SUB * i
            p = span * (r // block) + 2 * w * k
            q = r % block
            parts.append(pltpu.roll(ed[q:q + SUB], (cols - p) % cols, 1))
        return jnp.concatenate(parts, axis=0)

    def empty(w):
        return [jnp.zeros((SUB, cols), jnp.float32) for _ in range(geometry(w)[1] // SUB)]

    def halo_copies(e, g, w):
        i = e * groups + g
        sx, rx, sp, rp = (
            (xs.at[i], xr.at[i], ps.at[i], pr.at[i]) if w == 1
            else (xs2.at[g], xr2.at[g], ps2.at[g], pr2.at[g])
        )
        plan = (
            (sp, rp.at[0], at(gx, right)),
            (sp, rp.at[1], at(gx, left)),
            (sx.at[0], rx.at[1], at(up, gy)),
            (sx.at[1], rx.at[0], at(down, gy)),
        )
        return [
            pltpu.make_async_remote_copy(
                src_ref=s, dst_ref=r, send_sem=hs_sem.at[i, j], recv_sem=hr_sem.at[i, j],
                device_id=dev, device_id_type=MESH,
            )
            for j, (s, r, dev) in enumerate(plan)
        ]

    def send_halo(e, g, w, accs):
        i = e * groups + g
        ref = ps.at[i] if w == 1 else ps2.at[g]
        for q, v in enumerate(accs):
            ref[SUB * q:SUB * q + SUB, :] = v
        for c in halo_copies(e, g, w):
            c.start()

    def take_halo(e, g, w, field):
        i = e * groups + g
        for c in halo_copies(e, g, w):
            c.wait_recv()
        rx, rp = (xr.at[i], pr.at[i]) if w == 1 else (xr2.at[g], pr2.at[g])
        for k in range(GROUP):
            for j in range(w):
                m = j * GROUP + k
                field[g * GROUP + k, PAD - w + j:PAD - w + j + 1, :] = rx[0, m:m + 1, :]
                field[g * GROUP + k, PAD + rows + j:PAD + rows + j + 1, :] = rx[1, m:m + 1, :]
        size = geometry(w)[1]
        lanes = lax.broadcasted_iota(jnp.int32, (size, cols), 1)
        return jnp.where(
            lax.rem(lanes, 2 * w) < w, rp[0], pltpu.roll(rp[1], cols - 2 * w, 1)
        )

    def edge_rows(e, g, k, w, first, last):
        i = e * groups + g
        ref = xs.at[i] if w == 1 else xs2.at[g]
        for j in range(w):
            m = j * GROUP + k
            ref[0, m:m + 1, :] = first[j:j + 1]
            ref[1, m:m + 1, :] = last[CHUNK - w + j:CHUNK - w + j + 1]

    def fold(x):
        return jnp.sum(x.reshape(CHUNK // SUB, SUB, cols), axis=0)

    def put(acc, place, part):
        return jnp.where(sub == place, jnp.sum(part, axis=0, keepdims=True), acc)

    def send_sums(s, g, acc):
        i = s * groups + g
        line = jnp.sum(acc, axis=1, keepdims=True)
        row = jnp.sum(jnp.where(lane == sub, line, 0.0), axis=0, keepdims=True)
        ar_out[i] = row
        ar_in[i, me] = row

        def send(dev):
            pltpu.make_async_remote_copy(
                src_ref=ar_out.at[i], dst_ref=ar_in.at[i, me],
                send_sem=as_sem.at[i], recv_sem=ar_sem.at[i],
                device_id=dev, device_id_type=MESH,
            ).start()

        each_peer(send)

    def take_sums(s, g):
        i = s * groups + g
        got = ar_in.at[i, pl.ds(0, n - 1)]
        pltpu.make_async_copy(got, got, ar_sem.at[i]).wait()
        total = jnp.sum(ar_in[i], axis=0)
        line = jnp.sum(jnp.where(lane == sub, total, 0.0), axis=1, keepdims=True)
        return jnp.broadcast_to(line, (SUB, cols))

    def offset_of(g, total):
        return (total - lam_tab[g] * pltpu.roll(total, GROUP, 0)) * (1.0 / cells)

    starts = range(0, rows, CHUNK)
    zero8 = jnp.zeros((SUB, cols), jnp.float32)

    load_d.wait()
    load_c.wait()

    def begin(g, carry):
        def mix(r8, carry):
            r = pl.multiple_of(r8 * SUB, SUB)
            totals = [src[g * GROUP + k, pl.ds(r, SUB), :] for k in range(GROUP)]
            for j in range(classes):
                part = d[0, j, pl.ds(PAD + r, SUB), :]
                for k in range(GROUP):
                    totals[k] = totals[k] + coupling[g * GROUP + k, j] * part
            for k in range(GROUP):
                src[g * GROUP + k, pl.ds(r, SUB), :] = totals[k]
            return carry

        lax.fori_loop(0, rows // SUB, mix, 0, unroll=2)
        acc, accs, accs_d = zero8, empty(1), empty(1)
        for k in range(GROUP):
            kk = g * GROUP + k
            total = zero8
            ts, ds = [], []
            for r0 in starts:
                t = src[kk, r0:r0 + CHUNK, :] * 0.5
                dd = d[0, kk, PAD + r0:PAD + r0 + CHUNK, :]
                u[kk, PAD + r0:PAD + r0 + CHUNK, :] = t
                accs = pack(accs, t, k, r0, 1)
                accs_d = pack(accs_d, dd, k, r0, 1)
                total = total + fold(t)
                ts.append(t)
                ds.append(dd)
            edge_rows(1, g, k, 1, ts[0], ts[-1])
            edge_rows(0, g, k, 1, ds[0], ds[-1])
            acc = put(acc, k, total)
        lam_tab[g] = zero8

        @pl.when(g == 0)
        def _():
            pl.semaphore_wait(barrier, n - 1)

        send_halo(1, g, 1, accs)
        send_sums(0, g, acc)
        send_halo(0, g, 1, accs_d)
        return carry

    lax.fori_loop(0, groups, begin, 0)

    def neighbours(field, ed, kk, k, r0):
        lo = PAD + r0
        mid = field[kk, lo:lo + CHUNK, :]
        xp = field[kk, lo + 1:lo + 1 + CHUNK, :]
        xm = field[kk, lo - 1:lo - 1 + CHUNK, :]
        side = unpack(ed, k, r0, 1)
        yp = jnp.where(lane_c == cols - 1, side, pltpu.roll(mid, cols - 1, 1))
        ym = jnp.where(lane_c == 0, side, pltpu.roll(mid, 1, 1))
        return xp, xm, yp, ym

    def climb(s, g, w):
        ed = take_halo(s, g, 1, u)
        acc = zero8
        for k in range(GROUP):
            kk = g * GROUP + k
            sum_a, sum_b = zero8, zero8
            for r0 in starts:
                xp, xm, yp, ym = neighbours(u, ed, kk, k, r0)
                px = jnp.abs(xp - xm) * 0.5
                py = jnp.abs(yp - ym) * 0.5
                sx, sy = xp + xm, yp + ym
                inv = 1.0 / (2.0 + px + py)
                gain = (sx + sy) + px * (sx - px) + py * (sy - py)
                at_a = (src[kk, r0:r0 + CHUNK, :] + 0.5 * gain) * inv
                a[kk, r0:r0 + CHUNK, :] = at_a
                b[kk, r0:r0 + CHUNK, :] = inv
                sum_a = sum_a + fold(at_a)
                sum_b = sum_b + fold(inv)
            acc = put(put(acc, k, sum_a), GROUP + k, sum_b)
        send_sums(s, g, acc)
        lam_tab[g] = THETA * offset_of(g, take_sums(s - 1, g))
        accs = empty(w)
        for k in range(GROUP):
            kk = g * GROUP + k
            scale = lam_tab[g, k:k + 1, :]
            ts = []
            for r0 in starts:
                t = a[kk, r0:r0 + CHUNK, :] - scale * b[kk, r0:r0 + CHUNK, :]
                u[kk, PAD + r0:PAD + r0 + CHUNK, :] = t
                if w == 2:
                    trial[kk, r0:r0 + CHUNK, :] = t
                accs = pack(accs, t, k, r0, w)
                ts.append(t)
            edge_rows(s + 1, g, k, w, ts[0], ts[-1])
        send_halo(s + 1, g, w, accs)

    def middle(i, carry):
        climb(1 + i // groups, lax.rem(i, groups), 1)
        return carry

    def final(g, carry):
        climb(SWEEPS - 1, g, 2)
        return carry

    lax.fori_loop(0, (SWEEPS - 2) * groups, middle, 0)
    lax.fori_loop(0, groups, final, 0)

    base = SWEEPS + 1

    def weigh(g, carry):
        ed2 = take_halo(SWEEPS, g, 2, u)
        ed = take_halo(0, g, 1, d.at[0])
        lanes2 = lax.broadcasted_iota(jnp.int32, ed2.shape, 1)
        ed3 = jnp.where(
            lax.rem(lanes2, 4) < 2, pltpu.roll(ed2, cols - 1, 1), pltpu.roll(ed2, 1, 1)
        )
        accs = empty(1)
        for k in range(GROUP):
            kk = g * GROUP + k
            fs = []
            for r0 in starts:
                lo = PAD + r0
                mid = u[kk, lo:lo + CHUNK, :]
                xp = u[kk, lo + 1:lo + 1 + CHUNK, :]
                xm = u[kk, lo - 1:lo - 1 + CHUNK, :]
                xpp = u[kk, lo + 2:lo + 2 + CHUNK, :]
                xmm = u[kk, lo - 2:lo - 2 + CHUNK, :]
                side = unpack(ed2, k, r0, 2)
                near = unpack(ed3, k, r0, 2)
                ypp = jnp.where(lane_c >= cols - 2, side, pltpu.roll(mid, cols - 2, 1))
                ymm = jnp.where(lane_c < 2, side, pltpu.roll(mid, 2, 1))
                yp = jnp.where(lane_c == cols - 1, near, pltpu.roll(mid, cols - 1, 1))
                ym = jnp.where(lane_c == 0, near, pltpu.roll(mid, 1, 1))
                half = 0.5 / (2.0 + 0.5 * (jnp.abs(xp - xm) + jnp.abs(yp - ym)))
                c = [half * (1.0 + jnp.maximum(far - mid, 0.0)) for far in (xpp, xmm, ypp, ymm)]
                for ref, v in zip((cxp, cxm, cyp, cym), c):
                    ref[kk, r0:r0 + CHUNK, :] = v
                xp, xm, yp, ym = neighbours(d.at[0], ed, kk, k, r0)
                f = c[0] * xp + c[1] * xm + c[2] * yp + c[3] * ym
                d[1, kk, lo:lo + CHUNK, :] = f
                accs = pack(accs, f, k, r0, 1)
                fs.append(f)
            edge_rows(base, g, k, 1, fs[0], fs[-1])
        send_halo(base, g, 1, accs)
        return carry

    lax.fori_loop(0, groups, weigh, 0)

    def flow(s, g, last):
        now, then = lax.rem(s, 2), lax.rem(s + 1, 2)
        ed = take_halo(base + s - 1, g, 1, d.at[now])
        accs, acc = empty(1), zero8
        for k in range(GROUP):
            kk = g * GROUP + k
            fs, total = [], zero8
            for r0 in starts:
                c = [ref[kk, r0:r0 + CHUNK, :] for ref in (cxp, cxm, cyp, cym)]
                xp, xm, yp, ym = neighbours(d.at[now], ed, kk, k, r0)
                f = c[0] * xp + c[1] * xm + c[2] * yp + c[3] * ym
                if last:
                    fresh[kk, r0:r0 + CHUNK, :] = f
                    total = total + fold(f)
                else:
                    d[then, kk, PAD + r0:PAD + r0 + CHUNK, :] = f
                    accs = pack(accs, f, k, r0, 1)
                    fs.append(f)
            if last:
                acc = put(acc, k, total)
            else:
                edge_rows(base + s, g, k, 1, fs[0], fs[-1])
        if last:
            send_sums(SWEEPS, g, acc)
        else:
            send_halo(base + s, g, 1, accs)

    def flows(i, carry):
        flow(1 + i // groups, lax.rem(i, groups), False)
        return carry

    def last_flow(g, carry):
        flow(SWEEPS - 1, g, True)
        return carry

    lax.fori_loop(0, (SWEEPS - 2) * groups, flows, 0)
    lax.fori_loop(0, groups, last_flow, 0)

    def flat(g, line, row):
        mine = (lane == g * GROUP + sub) & (sub < GROUP)
        return row + jnp.sum(jnp.where(mine, line, 0.0), axis=0, keepdims=True)

    def shifts(g, row):
        return flat(g, offset_of(g, take_sums(SWEEPS - 1, g)), row)

    def drain(i, carry):
        for c in halo_copies(i // groups, lax.rem(i, groups), 1):
            c.wait_send()
        return carry

    def drain2(g, carry):
        for c in halo_copies(SWEEPS, g, 2):
            c.wait_send()
        return carry

    def drain_sums(i, carry):
        got = ar_in.at[i, pl.ds(0, n - 1)]
        pltpu.make_async_copy(got, got, as_sem.at[i]).wait()
        return carry

    zero_row = jnp.zeros((1, cols), jnp.float32)
    means[0:1, :] = lax.fori_loop(0, groups, shifts, zero_row)
    lax.fori_loop(0, SWEEPS * groups, drain, 0)
    lax.fori_loop(0, groups, drain2, 0)
    lax.fori_loop((SWEEPS + 1) * groups, 2 * SWEEPS * groups, drain, 0)
    lax.fori_loop(0, (SWEEPS + 1) * groups, drain_sums, 0)

    def masses(g, row):
        return flat(g, take_sums(SWEEPS, g) * (1.0 / cells), row)

    means[1:2, :] = lax.fori_loop(0, groups, masses, zero_row)


def shards(cost, density_start, coupling):
    nx, ny = lax.axis_size("gx"), lax.axis_size("gy")
    classes, rows, cols = cost.shape
    f32 = jnp.float32
    n = nx * ny
    groups = classes // GROUP
    full = pltpu.VMEM((classes, rows, cols), f32)
    slots = 2 * SWEEPS * groups
    sums = (SWEEPS + 1) * groups
    block = rows * 2 * GROUP // cols
    trial, fresh, means = pl.pallas_call(
        functools.partial(kernel, nx, ny),
        out_shape=(
            jax.ShapeDtypeStruct(cost.shape, f32),
            jax.ShapeDtypeStruct(cost.shape, f32),
            jax.ShapeDtypeStruct((2, cols), f32),
        ),
        in_specs=[
            pl.BlockSpec(memory_space=pl.ANY),
            pl.BlockSpec(memory_space=pl.ANY),
            pl.BlockSpec(memory_space=pltpu.SMEM),
        ],
        out_specs=(
            pl.BlockSpec(memory_space=pltpu.VMEM),
            pl.BlockSpec(memory_space=pltpu.VMEM),
            pl.BlockSpec(memory_space=pltpu.VMEM),
        ),
        scratch_shapes=[
            full, pltpu.VMEM((classes, rows + 2 * PAD, cols), f32), full, full,
            pltpu.VMEM((2, classes, rows + 2 * PAD, cols), f32), full, full, full, full,
            pltpu.VMEM((slots, 2, GROUP, cols), f32),
            pltpu.VMEM((slots, 2, GROUP, cols), f32),
            pltpu.VMEM((slots, block, cols), f32),
            pltpu.VMEM((slots, 2, block, cols), f32),
            pltpu.VMEM((groups, 2, 2 * GROUP, cols), f32),
            pltpu.VMEM((groups, 2, 2 * GROUP, cols), f32),
            pltpu.VMEM((groups, 2 * block, cols), f32),
            pltpu.VMEM((groups, 2, 2 * block, cols), f32),
            pltpu.VMEM((sums, 1, cols), f32),
            pltpu.VMEM((sums, n, 1, cols), f32),
            pltpu.VMEM((groups, SUB, cols), f32),
            pltpu.SemaphoreType.DMA((2,)),
            pltpu.SemaphoreType.DMA((slots, 4)),
            pltpu.SemaphoreType.DMA((slots, 4)),
            pltpu.SemaphoreType.DMA((sums,)),
            pltpu.SemaphoreType.DMA((sums,)),
        ],
        compiler_params=pltpu.CompilerParams(
            collective_id=0, has_side_effects=True, vmem_limit_bytes=VMEM_LIMIT
        ),
    )(cost, density_start, coupling)
    offset = means[0, :classes]
    mass = means[1, :classes]
    value = trial - offset[:, None, None]
    density = fresh / mass[:, None, None]
    return value, density, THETA * offset


VMEM_LIMIT = 67043328


def solution(mesh):
    placed = P(None, "gx", "gy")
    return jax.shard_map(
        shards,
        mesh=mesh,
        in_specs=(placed, placed, P()),
        out_specs=(placed, placed, P()),
        check_vma=False,
    )
```

```python
import functools

import jax
import jax.numpy as jnp
from jax import lax
from jax.experimental import pallas as pl
from jax.experimental.pallas import tpu as pltpu
from jax.sharding import PartitionSpec as P

MESH = pl.DeviceIdType.MESH
SWEEPS = 5
THETA = 2.0
PAD = 8
CHUNK = 32
SUB = 8
GROUP = 4


def kernel(
    nx, ny,
    cost_hbm, dens_hbm, coup_hbm,
    trial, fresh, means,
    coupling, src, u, a, b, d0, d1, cxp, cxm, cyp, cym,
    xs, xr, ps, pr, xs2, xr2, ps2, pr2,
    ar_out, ar_in, lam_tab,
    in_sem, hs_sem, hr_sem, as_sem, ar_sem,
):
    classes, rows, cols = cost_hbm.shape
    groups = classes // GROUP
    n = nx * ny
    cells = float(n * rows * cols)
    gx, gy = lax.axis_index("gx"), lax.axis_index("gy")
    up, down = lax.rem(gx + nx - 1, nx), lax.rem(gx + 1, nx)
    left, right = lax.rem(gy + ny - 1, ny), lax.rem(gy + 1, ny)
    me = gx * ny + gy

    def at(x, y):
        return {"gx": x, "gy": y}

    def each_peer(body):
        def step(i, carry):
            dx, dy = i // ny, lax.rem(i, ny)
            body(at(lax.rem(gx + dx, nx), lax.rem(gy + dy, ny)))
            return carry

        lax.fori_loop(1, n, step, 0, unroll=n - 1 if n <= 32 else 1)

    load_d = pltpu.make_async_copy(dens_hbm, d0.at[:, pl.ds(PAD, rows), :], in_sem.at[0])
    load_c = pltpu.make_async_copy(cost_hbm, src, in_sem.at[1])
    load_k = pltpu.make_async_copy(coup_hbm, coupling, in_sem.at[2])
    load_d.start()
    load_c.start()
    load_k.start()

    barrier = pltpu.get_barrier_semaphore()
    each_peer(lambda dev: pl.semaphore_signal(barrier, inc=1, device_id=dev, device_id_type=MESH))

    lane = lax.broadcasted_iota(jnp.int32, (SUB, cols), 1)
    sub = lax.broadcasted_iota(jnp.int32, (SUB, cols), 0)
    lane_c = lax.broadcasted_iota(jnp.int32, (CHUNK, cols), 1)
    pair = {w: lane // (2 * w) for w in (1, 2)}

    def geometry(w):
        span = 2 * w * GROUP
        return span, rows // (cols // span)

    def pack(accs, t, k, r0, w):
        span, block = geometry(w)
        accs = list(accs)
        for i in range(CHUNK // SUB):
            r = r0 + SUB * i
            p = span * (r // block) + 2 * w * k
            q = (r % block) // SUB
            turned = pltpu.roll(t[SUB * i:SUB * i + SUB], (p + w) % cols, 1)
            accs[q] = jnp.where(pair[w] == p // (2 * w), turned, accs[q])
        return accs

    def unpack(ed, k, r0, w):
        span, block = geometry(w)
        parts = []
        for i in range(CHUNK // SUB):
            r = r0 + SUB * i
            p = span * (r // block) + 2 * w * k
            q = r % block
            parts.append(pltpu.roll(ed[q:q + SUB], (cols - p) % cols, 1))
        return jnp.concatenate(parts, axis=0)

    def empty(w):
        return [jnp.zeros((SUB, cols), jnp.float32) for _ in range(geometry(w)[1] // SUB)]

    def halo_copies(e, g, w):
        i = e * groups + g
        sx, rx, sp, rp = (
            (xs.at[i], xr.at[i], ps.at[i], pr.at[i]) if w == 1
            else (xs2.at[g], xr2.at[g], ps2.at[g], pr2.at[g])
        )
        plan = (
            (sp, rp.at[0], at(gx, right)),
            (sp, rp.at[1], at(gx, left)),
            (sx.at[0], rx.at[1], at(up, gy)),
            (sx.at[1], rx.at[0], at(down, gy)),
        )
        return [
            pltpu.make_async_remote_copy(
                src_ref=s, dst_ref=r, send_sem=hs_sem.at[i, j], recv_sem=hr_sem.at[i, j],
                device_id=dev, device_id_type=MESH,
            )
            for j, (s, r, dev) in enumerate(plan)
        ]

    def send_halo(e, g, w, accs):
        i = e * groups + g
        ref = ps.at[i] if w == 1 else ps2.at[g]
        for q, v in enumerate(accs):
            ref[SUB * q:SUB * q + SUB, :] = v
        for c in halo_copies(e, g, w):
            c.start()

    def take_halo(e, g, w, field):
        i = e * groups + g
        for c in halo_copies(e, g, w):
            c.wait_recv()
        rx, rp = (xr.at[i], pr.at[i]) if w == 1 else (xr2.at[g], pr2.at[g])
        for k in range(GROUP):
            for j in range(w):
                m = j * GROUP + k
                field[g * GROUP + k, PAD - w + j:PAD - w + j + 1, :] = rx[0, m:m + 1, :]
                field[g * GROUP + k, PAD + rows + j:PAD + rows + j + 1, :] = rx[1, m:m + 1, :]
        size = geometry(w)[1]
        lanes = lax.broadcasted_iota(jnp.int32, (size, cols), 1)
        return jnp.where(
            lax.rem(lanes, 2 * w) < w, rp[0], pltpu.roll(rp[1], cols - 2 * w, 1)
        )

    def edge_rows(e, g, k, w, first, last):
        i = e * groups + g
        ref = xs.at[i] if w == 1 else xs2.at[g]
        for j in range(w):
            m = j * GROUP + k
            ref[0, m:m + 1, :] = first[j:j + 1]
            ref[1, m:m + 1, :] = last[CHUNK - w + j:CHUNK - w + j + 1]

    def fold(x):
        return jnp.sum(x.reshape(CHUNK // SUB, SUB, cols), axis=0)

    def put(acc, place, part):
        return jnp.where(sub == place, jnp.sum(part, axis=0, keepdims=True), acc)

    def send_sums(s, g, acc):
        i = s * groups + g
        line = jnp.sum(acc, axis=1, keepdims=True)
        row = jnp.sum(jnp.where(lane == sub, line, 0.0), axis=0, keepdims=True)
        ar_out[i] = row
        ar_in[i, me] = row

        def send(dev):
            pltpu.make_async_remote_copy(
                src_ref=ar_out.at[i], dst_ref=ar_in.at[i, me],
                send_sem=as_sem.at[i], recv_sem=ar_sem.at[i],
                device_id=dev, device_id_type=MESH,
            ).start()

        each_peer(send)

    def take_sums(s, g):
        i = s * groups + g
        got = ar_in.at[i, pl.ds(0, n - 1)]
        pltpu.make_async_copy(got, got, ar_sem.at[i]).wait()
        total = jnp.sum(ar_in[i], axis=0)
        line = jnp.sum(jnp.where(lane == sub, total, 0.0), axis=1, keepdims=True)
        return jnp.broadcast_to(line, (SUB, cols))

    def offset_of(g, total):
        return (total - lam_tab[g] * pltpu.roll(total, GROUP, 0)) * (1.0 / cells)

    starts = range(0, rows, CHUNK)
    zero8 = jnp.zeros((SUB, cols), jnp.float32)

    load_d.wait()
    load_c.wait()
    load_k.wait()

    def begin(g, carry):
        def mix(r8, carry):
            r = pl.multiple_of(r8 * SUB, SUB)
            totals = [src[g * GROUP + k, pl.ds(r, SUB), :] for k in range(GROUP)]
            for j in range(classes):
                part = d0[j, pl.ds(PAD + r, SUB), :]
                for k in range(GROUP):
                    totals[k] = totals[k] + coupling[g * GROUP + k, j] * part
            for k in range(GROUP):
                src[g * GROUP + k, pl.ds(r, SUB), :] = totals[k]
            return carry

        lax.fori_loop(0, rows // SUB, mix, 0, unroll=2)
        acc, accs, accs_d = zero8, empty(1), empty(1)
        for k in range(GROUP):
            kk = g * GROUP + k
            total = zero8
            ts, ds = [], []
            for r0 in starts:
                t = src[kk, r0:r0 + CHUNK, :] * 0.5
                dd = d0[kk, PAD + r0:PAD + r0 + CHUNK, :]
                u[kk, PAD + r0:PAD + r0 + CHUNK, :] = t
                accs = pack(accs, t, k, r0, 1)
                accs_d = pack(accs_d, dd, k, r0, 1)
                total = total + fold(t)
                ts.append(t)
                ds.append(dd)
            edge_rows(1, g, k, 1, ts[0], ts[-1])
            edge_rows(0, g, k, 1, ds[0], ds[-1])
            acc = put(acc, k, total)
        lam_tab[g] = zero8

        @pl.when(g == 0)
        def _():
            pl.semaphore_wait(barrier, n - 1)

        send_halo(1, g, 1, accs)
        send_sums(0, g, acc)
        send_halo(0, g, 1, accs_d)
        return carry

    lax.fori_loop(0, groups, begin, 0)

    def neighbours(field, ed, kk, k, r0):
        lo = PAD + r0
        mid = field[kk, lo:lo + CHUNK, :]
        xp = field[kk, lo + 1:lo + 1 + CHUNK, :]
        xm = field[kk, lo - 1:lo - 1 + CHUNK, :]
        side = unpack(ed, k, r0, 1)
        yp = jnp.where(lane_c == cols - 1, side, pltpu.roll(mid, cols - 1, 1))
        ym = jnp.where(lane_c == 0, side, pltpu.roll(mid, 1, 1))
        return xp, xm, yp, ym

    def climb(s, g, w):
        ed = take_halo(s, g, 1, u)
        acc = zero8
        for k in range(GROUP):
            kk = g * GROUP + k
            sum_a, sum_b = zero8, zero8
            for r0 in starts:
                xp, xm, yp, ym = neighbours(u, ed, kk, k, r0)
                px = jnp.abs(xp - xm) * 0.5
                py = jnp.abs(yp - ym) * 0.5
                sx, sy = xp + xm, yp + ym
                inv = 1.0 / (2.0 + px + py)
                gain = (sx + sy) + px * (sx - px) + py * (sy - py)
                at_a = (src[kk, r0:r0 + CHUNK, :] + 0.5 * gain) * inv
                a[kk, r0:r0 + CHUNK, :] = at_a
                b[kk, r0:r0 + CHUNK, :] = inv
                sum_a = sum_a + fold(at_a)
                sum_b = sum_b + fold(inv)
            acc = put(put(acc, k, sum_a), GROUP + k, sum_b)
        send_sums(s, g, acc)
        lam_tab[g] = THETA * offset_of(g, take_sums(s - 1, g))
        accs = empty(w)
        for k in range(GROUP):
            kk = g * GROUP + k
            scale = lam_tab[g, k:k + 1, :]
            ts = []
            for r0 in starts:
                t = a[kk, r0:r0 + CHUNK, :] - scale * b[kk, r0:r0 + CHUNK, :]
                u[kk, PAD + r0:PAD + r0 + CHUNK, :] = t
                if w == 2:
                    trial[kk, r0:r0 + CHUNK, :] = t
                accs = pack(accs, t, k, r0, w)
                ts.append(t)
            edge_rows(s + 1, g, k, w, ts[0], ts[-1])
        send_halo(s + 1, g, w, accs)

    def middle(i, carry):
        climb(1 + i // groups, lax.rem(i, groups), 1)
        return carry

    def final(g, carry):
        climb(SWEEPS - 1, g, 2)
        return carry

    lax.fori_loop(0, (SWEEPS - 2) * groups, middle, 0)
    lax.fori_loop(0, groups, final, 0)

    base = SWEEPS + 1

    def weigh(g, carry):
        ed2 = take_halo(SWEEPS, g, 2, u)
        ed = take_halo(0, g, 1, d0)
        lanes2 = lax.broadcasted_iota(jnp.int32, ed2.shape, 1)
        ed3 = jnp.where(
            lax.rem(lanes2, 4) < 2, pltpu.roll(ed2, cols - 1, 1), pltpu.roll(ed2, 1, 1)
        )
        accs = empty(1)
        for k in range(GROUP):
            kk = g * GROUP + k
            fs = []
            for r0 in starts:
                lo = PAD + r0
                mid = u[kk, lo:lo + CHUNK, :]
                xp = u[kk, lo + 1:lo + 1 + CHUNK, :]
                xm = u[kk, lo - 1:lo - 1 + CHUNK, :]
                xpp = u[kk, lo + 2:lo + 2 + CHUNK, :]
                xmm = u[kk, lo - 2:lo - 2 + CHUNK, :]
                side = unpack(ed2, k, r0, 2)
                near = unpack(ed3, k, r0, 2)
                ypp = jnp.where(lane_c >= cols - 2, side, pltpu.roll(mid, cols - 2, 1))
                ymm = jnp.where(lane_c < 2, side, pltpu.roll(mid, 2, 1))
                yp = jnp.where(lane_c == cols - 1, near, pltpu.roll(mid, cols - 1, 1))
                ym = jnp.where(lane_c == 0, near, pltpu.roll(mid, 1, 1))
                half = 0.5 / (2.0 + 0.5 * (jnp.abs(xp - xm) + jnp.abs(yp - ym)))
                c = [half * (1.0 + jnp.maximum(far - mid, 0.0)) for far in (xpp, xmm, ypp, ymm)]
                for ref, v in zip((cxp, cxm, cyp, cym), c):
                    ref[kk, r0:r0 + CHUNK, :] = v
                xp, xm, yp, ym = neighbours(d0, ed, kk, k, r0)
                f = c[0] * xp + c[1] * xm + c[2] * yp + c[3] * ym
                d1[kk, lo:lo + CHUNK, :] = f
                accs = pack(accs, f, k, r0, 1)
                fs.append(f)
            edge_rows(base, g, k, 1, fs[0], fs[-1])
        send_halo(base, g, 1, accs)
        return carry

    lax.fori_loop(0, groups, weigh, 0)

    def flow(s, g, last):
        now, then = (d1, d0) if s % 2 else (d0, d1)
        ed = take_halo(base + s - 1, g, 1, now)
        accs, acc = empty(1), zero8
        for k in range(GROUP):
            kk = g * GROUP + k
            fs, total = [], zero8
            for r0 in starts:
                c = [ref[kk, r0:r0 + CHUNK, :] for ref in (cxp, cxm, cyp, cym)]
                xp, xm, yp, ym = neighbours(now, ed, kk, k, r0)
                f = c[0] * xp + c[1] * xm + c[2] * yp + c[3] * ym
                if last:
                    fresh[kk, r0:r0 + CHUNK, :] = f
                    total = total + fold(f)
                else:
                    then[kk, PAD + r0:PAD + r0 + CHUNK, :] = f
                    accs = pack(accs, f, k, r0, 1)
                    fs.append(f)
            if last:
                acc = put(acc, k, total)
            else:
                edge_rows(base + s, g, k, 1, fs[0], fs[-1])
        if last:
            send_sums(SWEEPS, g, acc)
        else:
            send_halo(base + s, g, 1, accs)

    for s in range(1, SWEEPS):

        def flows(g, carry):
            flow(s, g, s == SWEEPS - 1)
            return carry

        lax.fori_loop(0, groups, flows, 0)

    def flat(g, line, row):
        mine = (lane == g * GROUP + sub) & (sub < GROUP)
        return row + jnp.sum(jnp.where(mine, line, 0.0), axis=0, keepdims=True)

    def shifts(g, row):
        return flat(g, offset_of(g, take_sums(SWEEPS - 1, g)), row)

    def drain(i, carry):
        for c in halo_copies(i // groups, lax.rem(i, groups), 1):
            c.wait_send()
        return carry

    def drain2(g, carry):
        for c in halo_copies(SWEEPS, g, 2):
            c.wait_send()
        return carry

    def drain_sums(i, carry):
        got = ar_in.at[i, pl.ds(0, n - 1)]
        pltpu.make_async_copy(got, got, as_sem.at[i]).wait()
        return carry

    zero_row = jnp.zeros((1, cols), jnp.float32)
    means[0:1, :] = lax.fori_loop(0, groups, shifts, zero_row)
    lax.fori_loop(0, SWEEPS * groups, drain, 0)
    lax.fori_loop(0, groups, drain2, 0)
    lax.fori_loop((SWEEPS + 1) * groups, 2 * SWEEPS * groups, drain, 0)
    lax.fori_loop(0, (SWEEPS + 1) * groups, drain_sums, 0)

    def masses(g, row):
        return flat(g, take_sums(SWEEPS, g) * (1.0 / cells), row)

    means[1:2, :] = lax.fori_loop(0, groups, masses, zero_row)


def shards(cost, density_start, coupling):
    nx, ny = lax.axis_size("gx"), lax.axis_size("gy")
    classes, rows, cols = cost.shape
    f32 = jnp.float32
    n = nx * ny
    groups = classes // GROUP
    full = pltpu.VMEM((classes, rows, cols), f32)
    padded = pltpu.VMEM((classes, rows + 2 * PAD, cols), f32)
    slots = 2 * SWEEPS * groups
    sums = (SWEEPS + 1) * groups
    block = rows * 2 * GROUP // cols
    trial, fresh, means = pl.pallas_call(
        functools.partial(kernel, nx, ny),
        out_shape=(
            jax.ShapeDtypeStruct(cost.shape, f32),
            jax.ShapeDtypeStruct(cost.shape, f32),
            jax.ShapeDtypeStruct((2, cols), f32),
        ),
        in_specs=[
            pl.BlockSpec(memory_space=pl.ANY),
            pl.BlockSpec(memory_space=pl.ANY),
            pl.BlockSpec(memory_space=pl.ANY),
        ],
        out_specs=(
            pl.BlockSpec(memory_space=pltpu.VMEM),
            pl.BlockSpec(memory_space=pltpu.VMEM),
            pl.BlockSpec(memory_space=pltpu.VMEM),
        ),
        scratch_shapes=[
            pltpu.SMEM(coupling.shape, f32),
            full, padded, full, full,
            padded, padded, full, full, full, full,
            pltpu.VMEM((slots, 2, GROUP, cols), f32),
            pltpu.VMEM((slots, 2, GROUP, cols), f32),
            pltpu.VMEM((slots, block, cols), f32),
            pltpu.VMEM((slots, 2, block, cols), f32),
            pltpu.VMEM((groups, 2, 2 * GROUP, cols), f32),
            pltpu.VMEM((groups, 2, 2 * GROUP, cols), f32),
            pltpu.VMEM((groups, 2 * block, cols), f32),
            pltpu.VMEM((groups, 2, 2 * block, cols), f32),
            pltpu.VMEM((sums, 1, cols), f32),
            pltpu.VMEM((sums, n, 1, cols), f32),
            pltpu.VMEM((groups, SUB, cols), f32),
            pltpu.SemaphoreType.DMA((3,)),
            pltpu.SemaphoreType.DMA((slots, 4)),
            pltpu.SemaphoreType.DMA((slots, 4)),
            pltpu.SemaphoreType.DMA((sums,)),
            pltpu.SemaphoreType.DMA((sums,)),
        ],
        compiler_params=pltpu.CompilerParams(
            collective_id=0, has_side_effects=True, vmem_limit_bytes=VMEM_LIMIT
        ),
    )(cost, density_start, coupling)
    offset = means[0, :classes]
    mass = means[1, :classes]
    value = trial - offset[:, None, None]
    density = fresh / mass[:, None, None]
    return value, density, THETA * offset


VMEM_LIMIT = 54000000


def solution(mesh):
    placed = P(None, "gx", "gy")
    return jax.shard_map(
        shards,
        mesh=mesh,
        in_specs=(placed, placed, P()),
        out_specs=(placed, placed, P()),
        check_vma=False,
    )
```

```python
import functools

import jax
import jax.numpy as jnp
from jax import lax
from jax.experimental import pallas as pl
from jax.experimental.pallas import tpu as pltpu
from jax.sharding import PartitionSpec as P

MESH = pl.DeviceIdType.MESH
SWEEPS = 5
THETA = 2.0
PAD = 8
CHUNK = 32
SUB = 8
GROUP = 4


def kernel(
    nx, ny,
    cost_hbm, dens_hbm, coup_hbm,
    trial, fresh, means,
    coupling, src, u, a, b, d0, d1, cxp, cxm, cyp, cym,
    xs, xr, ps, pr, xs2, xr2, ps2, pr2,
    ar_out, ar_in, lam_tab,
    in_sem, hs_sem, hr_sem, as_sem, ar_sem,
):
    classes, rows, cols = cost_hbm.shape
    groups = classes // GROUP
    n = nx * ny
    cells = float(n * rows * cols)
    gx, gy = lax.axis_index("gx"), lax.axis_index("gy")
    up, down = lax.rem(gx + nx - 1, nx), lax.rem(gx + 1, nx)
    left, right = lax.rem(gy + ny - 1, ny), lax.rem(gy + 1, ny)
    me = gx * ny + gy

    def at(x, y):
        return {"gx": x, "gy": y}

    def each_peer(body):
        def step(i, carry):
            dx, dy = i // ny, lax.rem(i, ny)
            body(at(lax.rem(gx + dx, nx), lax.rem(gy + dy, ny)))
            return carry

        lax.fori_loop(1, n, step, 0, unroll=n - 1 if n <= 32 else 1)

    load_d = pltpu.make_async_copy(dens_hbm, d0.at[:, pl.ds(PAD, rows), :], in_sem.at[0])
    load_c = pltpu.make_async_copy(cost_hbm, src, in_sem.at[1])
    load_k = pltpu.make_async_copy(coup_hbm, coupling, in_sem.at[2])
    load_d.start()
    load_c.start()
    load_k.start()

    barrier = pltpu.get_barrier_semaphore()
    each_peer(lambda dev: pl.semaphore_signal(barrier, inc=1, device_id=dev, device_id_type=MESH))

    lane = lax.broadcasted_iota(jnp.int32, (SUB, cols), 1)
    sub = lax.broadcasted_iota(jnp.int32, (SUB, cols), 0)
    lane_c = lax.broadcasted_iota(jnp.int32, (CHUNK, cols), 1)
    pair = {w: lane // (2 * w) for w in (1, 2)}

    def geometry(w):
        span = 2 * w * GROUP
        return span, rows // (cols // span)

    def pack(accs, t, k, r0, w):
        span, block = geometry(w)
        accs = list(accs)
        for i in range(CHUNK // SUB):
            r = r0 + SUB * i
            p = span * (r // block) + 2 * w * k
            q = (r % block) // SUB
            turned = pltpu.roll(t[SUB * i:SUB * i + SUB], (p + w) % cols, 1)
            accs[q] = jnp.where(pair[w] == p // (2 * w), turned, accs[q])
        return accs

    def unpack(ed, k, r0, w):
        span, block = geometry(w)
        parts = []
        for i in range(CHUNK // SUB):
            r = r0 + SUB * i
            p = span * (r // block) + 2 * w * k
            q = r % block
            parts.append(pltpu.roll(ed[q:q + SUB], (cols - p) % cols, 1))
        return jnp.concatenate(parts, axis=0)

    def empty(w):
        return [jnp.zeros((SUB, cols), jnp.float32) for _ in range(geometry(w)[1] // SUB)]

    def halo_copies(e, g, w):
        i = e * groups + g
        sx, rx, sp, rp = (
            (xs.at[i], xr.at[i], ps.at[i], pr.at[i]) if w == 1
            else (xs2.at[g], xr2.at[g], ps2.at[g], pr2.at[g])
        )
        plan = (
            (sp, rp.at[0], at(gx, right)),
            (sp, rp.at[1], at(gx, left)),
            (sx.at[0], rx.at[1], at(up, gy)),
            (sx.at[1], rx.at[0], at(down, gy)),
        )
        return [
            pltpu.make_async_remote_copy(
                src_ref=s, dst_ref=r, send_sem=hs_sem.at[i, j], recv_sem=hr_sem.at[i, j],
                device_id=dev, device_id_type=MESH,
            )
            for j, (s, r, dev) in enumerate(plan)
        ]

    def send_halo(e, g, w, accs):
        i = e * groups + g
        ref = ps.at[i] if w == 1 else ps2.at[g]
        for q, v in enumerate(accs):
            ref[SUB * q:SUB * q + SUB, :] = v
        for c in halo_copies(e, g, w):
            c.start()

    def take_halo(e, g, w, above, below):
        i = e * groups + g
        for c in halo_copies(e, g, w):
            c.wait_recv()
        rx, rp = (xr.at[i], pr.at[i]) if w == 1 else (xr2.at[g], pr2.at[g])
        for k in range(GROUP):
            for j in range(w):
                m = j * GROUP + k
                above[g * GROUP + k, PAD - w + j:PAD - w + j + 1, :] = rx[0, m:m + 1, :]
                below[g * GROUP + k, PAD + rows + j:PAD + rows + j + 1, :] = rx[1, m:m + 1, :]
        size = geometry(w)[1]
        lanes = lax.broadcasted_iota(jnp.int32, (size, cols), 1)
        return jnp.where(
            lax.rem(lanes, 2 * w) < w, rp[0], pltpu.roll(rp[1], cols - 2 * w, 1)
        )

    def edge_rows(e, g, k, w, first, last):
        i = e * groups + g
        ref = xs.at[i] if w == 1 else xs2.at[g]
        for j in range(w):
            m = j * GROUP + k
            ref[0, m:m + 1, :] = first[j:j + 1]
            ref[1, m:m + 1, :] = last[CHUNK - w + j:CHUNK - w + j + 1]

    def fold(x):
        return jnp.sum(x.reshape(CHUNK // SUB, SUB, cols), axis=0)

    def put(acc, place, part):
        return jnp.where(sub == place, jnp.sum(part, axis=0, keepdims=True), acc)

    def send_sums(s, g, acc):
        i = s * groups + g
        line = jnp.sum(acc, axis=1, keepdims=True)
        row = jnp.sum(jnp.where(lane == sub, line, 0.0), axis=0, keepdims=True)
        ar_out[i] = row
        ar_in[i, me] = row

        def send(dev):
            pltpu.make_async_remote_copy(
                src_ref=ar_out.at[i], dst_ref=ar_in.at[i, me],
                send_sem=as_sem.at[i], recv_sem=ar_sem.at[i],
                device_id=dev, device_id_type=MESH,
            ).start()

        each_peer(send)

    def take_sums(s, g):
        i = s * groups + g
        got = ar_in.at[i, pl.ds(0, n - 1)]
        pltpu.make_async_copy(got, got, ar_sem.at[i]).wait()
        total = jnp.sum(ar_in[i], axis=0)
        line = jnp.sum(jnp.where(lane == sub, total, 0.0), axis=1, keepdims=True)
        return jnp.broadcast_to(line, (SUB, cols))

    def offset_of(g, total):
        return (total - lam_tab[g] * pltpu.roll(total, GROUP, 0)) * (1.0 / cells)

    starts = range(0, rows, CHUNK)
    zero8 = jnp.zeros((SUB, cols), jnp.float32)

    load_d.wait()
    load_c.wait()
    load_k.wait()

    def begin(g, carry):
        def mix(r8, carry):
            r = pl.multiple_of(r8 * SUB, SUB)
            totals = [src[g * GROUP + k, pl.ds(r, SUB), :] for k in range(GROUP)]
            for j in range(classes):
                part = d0[j, pl.ds(PAD + r, SUB), :]
                for k in range(GROUP):
                    totals[k] = totals[k] + coupling[g * GROUP + k, j] * part
            for k in range(GROUP):
                src[g * GROUP + k, pl.ds(r, SUB), :] = totals[k]
            return carry

        lax.fori_loop(0, rows // SUB, mix, 0, unroll=2)
        acc, accs, accs_d = zero8, empty(1), empty(1)
        for k in range(GROUP):
            kk = g * GROUP + k
            total = zero8
            ts, ds = [], []
            for r0 in starts:
                t = src[kk, r0:r0 + CHUNK, :] * 0.5
                dd = d0[kk, PAD + r0:PAD + r0 + CHUNK, :]
                u[kk, PAD + r0:PAD + r0 + CHUNK, :] = t
                accs = pack(accs, t, k, r0, 1)
                accs_d = pack(accs_d, dd, k, r0, 1)
                total = total + fold(t)
                ts.append(t)
                ds.append(dd)
            edge_rows(1, g, k, 1, ts[0], ts[-1])
            edge_rows(0, g, k, 1, ds[0], ds[-1])
            acc = put(acc, k, total)
        lam_tab[g] = zero8

        @pl.when(g == 0)
        def _():
            pl.semaphore_wait(barrier, n - 1)

        send_halo(1, g, 1, accs)
        send_sums(0, g, acc)
        send_halo(0, g, 1, accs_d)
        return carry

    lax.fori_loop(0, groups, begin, 0)

    def neighbours(field, ed, kk, k, r0):
        lo = PAD + r0
        mid = field[kk, lo:lo + CHUNK, :]
        xp = field[kk, lo + 1:lo + 1 + CHUNK, :]
        xm = field[kk, lo - 1:lo - 1 + CHUNK, :]
        side = unpack(ed, k, r0, 1)
        yp = jnp.where(lane_c == cols - 1, side, pltpu.roll(mid, cols - 1, 1))
        ym = jnp.where(lane_c == 0, side, pltpu.roll(mid, 1, 1))
        return xp, xm, yp, ym

    def climb(s, g, w):
        ed = take_halo(s, g, 1, u, u)
        acc = zero8
        for k in range(GROUP):
            kk = g * GROUP + k
            sum_a, sum_b = zero8, zero8
            for r0 in starts:
                xp, xm, yp, ym = neighbours(u, ed, kk, k, r0)
                px = jnp.abs(xp - xm) * 0.5
                py = jnp.abs(yp - ym) * 0.5
                sx, sy = xp + xm, yp + ym
                inv = 1.0 / (2.0 + px + py)
                gain = (sx + sy) + px * (sx - px) + py * (sy - py)
                at_a = (src[kk, r0:r0 + CHUNK, :] + 0.5 * gain) * inv
                a[kk, r0:r0 + CHUNK, :] = at_a
                b[kk, r0:r0 + CHUNK, :] = inv
                sum_a = sum_a + fold(at_a)
                sum_b = sum_b + fold(inv)
            acc = put(put(acc, k, sum_a), GROUP + k, sum_b)
        send_sums(s, g, acc)
        lam_tab[g] = THETA * offset_of(g, take_sums(s - 1, g))
        accs = empty(w)
        for k in range(GROUP):
            kk = g * GROUP + k
            scale = lam_tab[g, k:k + 1, :]
            ts = []
            for r0 in starts:
                t = a[kk, r0:r0 + CHUNK, :] - scale * b[kk, r0:r0 + CHUNK, :]
                u[kk, PAD + r0:PAD + r0 + CHUNK, :] = t
                if w == 2:
                    trial[kk, r0:r0 + CHUNK, :] = t
                accs = pack(accs, t, k, r0, w)
                ts.append(t)
            edge_rows(s + 1, g, k, w, ts[0], ts[-1])
        send_halo(s + 1, g, w, accs)

    def middle(i, carry):
        climb(1 + i // groups, lax.rem(i, groups), 1)
        return carry

    def final(g, carry):
        climb(SWEEPS - 1, g, 2)
        return carry

    lax.fori_loop(0, (SWEEPS - 2) * groups, middle, 0)
    lax.fori_loop(0, groups, final, 0)

    base = SWEEPS + 1
    extra = 2 * SWEEPS

    def weights(g):
        ed2 = take_halo(SWEEPS, g, 2, u, u)
        lanes2 = lax.broadcasted_iota(jnp.int32, ed2.shape, 1)
        ed3 = jnp.where(
            lax.rem(lanes2, 4) < 2, pltpu.roll(ed2, cols - 1, 1), pltpu.roll(ed2, 1, 1)
        )
        for k in range(GROUP):
            kk = g * GROUP + k
            cs = []
            for r0 in starts:
                lo = PAD + r0
                mid = u[kk, lo:lo + CHUNK, :]
                xp = u[kk, lo + 1:lo + 1 + CHUNK, :]
                xm = u[kk, lo - 1:lo - 1 + CHUNK, :]
                xpp = u[kk, lo + 2:lo + 2 + CHUNK, :]
                xmm = u[kk, lo - 2:lo - 2 + CHUNK, :]
                side = unpack(ed2, k, r0, 2)
                near = unpack(ed3, k, r0, 2)
                ypp = jnp.where(lane_c >= cols - 2, side, pltpu.roll(mid, cols - 2, 1))
                ymm = jnp.where(lane_c < 2, side, pltpu.roll(mid, 2, 1))
                yp = jnp.where(lane_c == cols - 1, near, pltpu.roll(mid, cols - 1, 1))
                ym = jnp.where(lane_c == 0, near, pltpu.roll(mid, 1, 1))
                half = 0.5 / (2.0 + 0.5 * (jnp.abs(xp - xm) + jnp.abs(yp - ym)))
                c = [half * (1.0 + jnp.maximum(far - mid, 0.0)) for far in (xpp, xmm, ypp, ymm)]
                cxp[kk, lo:lo + CHUNK, :] = c[0]
                cxm[kk, lo:lo + CHUNK, :] = c[1]
                cyp[kk, r0:r0 + CHUNK, :] = c[2]
                cym[kk, r0:r0 + CHUNK, :] = c[3]
                cs.append(c)
            edge_rows(extra, g, k, 1, cs[0][1], cs[-1][0])

    def send_weights(g):
        accs = empty(1)
        for k in range(GROUP):
            kk = g * GROUP + k
            for r0 in starts:
                rim = jnp.where(lane_c == 0, cym[kk, r0:r0 + CHUNK, :], cyp[kk, r0:r0 + CHUNK, :])
                accs = pack(accs, rim, k, r0, 1)
        send_halo(extra, g, 1, accs)

    def flow(s, g):
        last, counted = s == SWEEPS - 1, s == SWEEPS - 2
        now, then = (d1, d0) if s % 2 else (d0, d1)
        ed = take_halo(base + s - 1 if s else 0, g, 1, now, now)
        accs, acc = empty(1), zero8
        for k in range(GROUP):
            kk = g * GROUP + k
            fs, total = [], zero8
            for r0 in starts:
                lo = PAD + r0
                c = [
                    cxp[kk, lo:lo + CHUNK, :], cxm[kk, lo:lo + CHUNK, :],
                    cyp[kk, r0:r0 + CHUNK, :], cym[kk, r0:r0 + CHUNK, :],
                ]
                xp, xm, yp, ym = neighbours(now, ed, kk, k, r0)
                f = c[0] * xp + c[1] * xm + c[2] * yp + c[3] * ym
                if last:
                    fresh[kk, r0:r0 + CHUNK, :] = f
                    continue
                then[kk, lo:lo + CHUNK, :] = f
                accs = pack(accs, f, k, r0, 1)
                fs.append(f)
                if counted:
                    total = total + fold(f * a[kk, r0:r0 + CHUNK, :])
            if not last:
                edge_rows(base + s, g, k, 1, fs[0], fs[-1])
            if counted:
                acc = put(acc, k, total)
        if not last:
            send_halo(base + s, g, 1, accs)
        if counted:
            send_sums(SWEEPS, g, acc)

    def shares(g):
        ed = take_halo(extra, g, 1, cxp, cxm)
        for k in range(GROUP):
            kk = g * GROUP + k
            for r0 in starts:
                lo = PAD + r0
                side = unpack(ed, k, r0, 1)
                east = pltpu.roll(cym[kk, r0:r0 + CHUNK, :], cols - 1, 1)
                west = pltpu.roll(cyp[kk, r0:r0 + CHUNK, :], 1, 1)
                a[kk, r0:r0 + CHUNK, :] = (
                    (cxp[kk, lo - 1:lo - 1 + CHUNK, :] + cxm[kk, lo + 1:lo + 1 + CHUNK, :])
                    + (jnp.where(lane_c == cols - 1, side, east) + jnp.where(lane_c == 0, side, west))
                )

    def flat(g, line, row):
        mine = (lane == g * GROUP + sub) & (sub < GROUP)
        return row + jnp.sum(jnp.where(mine, line, 0.0), axis=0, keepdims=True)

    def shifts(g, row):
        return flat(g, offset_of(g, take_sums(SWEEPS - 1, g)), row)

    def drain(i, carry):
        for c in halo_copies(i // groups, lax.rem(i, groups), 1):
            c.wait_send()
        return carry

    def drain2(g, carry):
        for c in halo_copies(SWEEPS, g, 2):
            c.wait_send()
        return carry

    def drain_sums(i, carry):
        got = ar_in.at[i, pl.ds(0, n - 1)]
        pltpu.make_async_copy(got, got, as_sem.at[i]).wait()
        return carry

    end = base + SWEEPS - 2
    for s in range(SWEEPS):

        def flows(g, carry):
            if s == 0:
                weights(g)
            flow(s, g)
            if s == 0:
                send_weights(g)
            if s == SWEEPS - 3:
                shares(g)
            return carry

        if s == SWEEPS - 1:
            means[0:1, :] = lax.fori_loop(0, groups, shifts, jnp.zeros((1, cols), jnp.float32))
            lax.fori_loop(0, SWEEPS * groups, drain, 0)
            lax.fori_loop(0, groups, drain2, 0)
            lax.fori_loop(base * groups, end * groups, drain, 0)
            lax.fori_loop(extra * groups, (extra + 1) * groups, drain, 0)
            lax.fori_loop(0, SWEEPS * groups, drain_sums, 0)
        lax.fori_loop(0, groups, flows, 0)

    lax.fori_loop(end * groups, (end + 1) * groups, drain, 0)
    row = jnp.zeros((1, cols), jnp.float32)
    for g in range(groups):
        i = SWEEPS * groups + g
        drain_sums(i, 0)
        got = ar_in.at[i, pl.ds(0, n - 1)]
        pltpu.make_async_copy(got, got, ar_sem.at[i]).wait()
        total = jnp.where(lane[0:1] < GROUP, jnp.sum(ar_in[i], axis=0), 0.0)
        row = row + (total if g == 0 else pltpu.roll(total, g * GROUP, 1))
    means[1:2, :] = row * (1.0 / cells)


def shards(cost, density_start, coupling):
    nx, ny = lax.axis_size("gx"), lax.axis_size("gy")
    classes, rows, cols = cost.shape
    f32 = jnp.float32
    n = nx * ny
    groups = classes // GROUP
    full = pltpu.VMEM((classes, rows, cols), f32)
    padded = pltpu.VMEM((classes, rows + 2 * PAD, cols), f32)
    slots = (2 * SWEEPS + 1) * groups
    sums = (SWEEPS + 1) * groups
    block = rows * 2 * GROUP // cols
    trial, fresh, means = pl.pallas_call(
        functools.partial(kernel, nx, ny),
        out_shape=(
            jax.ShapeDtypeStruct(cost.shape, f32),
            jax.ShapeDtypeStruct(cost.shape, f32),
            jax.ShapeDtypeStruct((2, cols), f32),
        ),
        in_specs=[
            pl.BlockSpec(memory_space=pl.ANY),
            pl.BlockSpec(memory_space=pl.ANY),
            pl.BlockSpec(memory_space=pl.ANY),
        ],
        out_specs=(
            pl.BlockSpec(memory_space=pltpu.VMEM),
            pl.BlockSpec(memory_space=pltpu.VMEM),
            pl.BlockSpec(memory_space=pltpu.VMEM),
        ),
        scratch_shapes=[
            pltpu.SMEM(coupling.shape, f32),
            full, padded, full, full,
            padded, padded, padded, padded, full, full,
            pltpu.VMEM((slots, 2, GROUP, cols), f32),
            pltpu.VMEM((slots, 2, GROUP, cols), f32),
            pltpu.VMEM((slots, block, cols), f32),
            pltpu.VMEM((slots, 2, block, cols), f32),
            pltpu.VMEM((groups, 2, 2 * GROUP, cols), f32),
            pltpu.VMEM((groups, 2, 2 * GROUP, cols), f32),
            pltpu.VMEM((groups, 2 * block, cols), f32),
            pltpu.VMEM((groups, 2, 2 * block, cols), f32),
            pltpu.VMEM((sums, 1, cols), f32),
            pltpu.VMEM((sums, n, 1, cols), f32),
            pltpu.VMEM((groups, SUB, cols), f32),
            pltpu.SemaphoreType.DMA((3,)),
            pltpu.SemaphoreType.DMA((slots, 4)),
            pltpu.SemaphoreType.DMA((slots, 4)),
            pltpu.SemaphoreType.DMA((sums,)),
            pltpu.SemaphoreType.DMA((sums,)),
        ],
        compiler_params=pltpu.CompilerParams(
            collective_id=0, has_side_effects=True, vmem_limit_bytes=VMEM_LIMIT
        ),
    )(cost, density_start, coupling)
    offset = means[0, :classes]
    mass = means[1, :classes]
    value = trial - offset[:, None, None]
    density = fresh / mass[:, None, None]
    return value, density, THETA * offset


VMEM_LIMIT = 54000000


def solution(mesh):
    placed = P(None, "gx", "gy")
    return jax.shard_map(
        shards,
        mesh=mesh,
        in_specs=(placed, placed, P()),
        out_specs=(placed, placed, P()),
        check_vma=False,
    )
```

```python
import functools

import jax
import jax.numpy as jnp
from jax import lax
from jax.experimental import pallas as pl
from jax.experimental.pallas import tpu as pltpu
from jax.sharding import PartitionSpec as P

MESH = pl.DeviceIdType.MESH
SWEEPS = 5
THETA = 2.0
PAD = 8
CHUNK = 32
SUB = 8
GROUP = 4


def kernel(
    nx, ny,
    cost_hbm, dens_hbm, coup_hbm,
    trial, fresh, means,
    coupling, src, u, a, b, d0, d1, cxp, cxm, cyp, cym,
    xs, xr, ps, pr, xs2, xr2, ps2, pr2,
    ar_out, ar_in, lam_tab,
    in_sem, hs_sem, hr_sem, as_sem, ar_sem,
):
    classes, rows, cols = cost_hbm.shape
    groups = classes // GROUP
    n = nx * ny
    cells = float(n * rows * cols)
    gx, gy = lax.axis_index("gx"), lax.axis_index("gy")
    up, down = lax.rem(gx + nx - 1, nx), lax.rem(gx + 1, nx)
    left, right = lax.rem(gy + ny - 1, ny), lax.rem(gy + 1, ny)
    me = gx * ny + gy

    def at(x, y):
        return {"gx": x, "gy": y}

    def each_peer(body):
        def step(i, carry):
            dx, dy = i // ny, lax.rem(i, ny)
            body(at(lax.rem(gx + dx, nx), lax.rem(gy + dy, ny)))
            return carry

        lax.fori_loop(1, n, step, 0, unroll=n - 1 if n <= 32 else 1)

    load_d = pltpu.make_async_copy(dens_hbm, d0.at[:, pl.ds(PAD, rows), :], in_sem.at[0])
    load_c = pltpu.make_async_copy(cost_hbm, src, in_sem.at[1])
    load_k = pltpu.make_async_copy(coup_hbm, coupling, in_sem.at[2])
    load_d.start()
    load_c.start()
    load_k.start()

    barrier = pltpu.get_barrier_semaphore()
    each_peer(lambda dev: pl.semaphore_signal(barrier, inc=1, device_id=dev, device_id_type=MESH))

    lane = lax.broadcasted_iota(jnp.int32, (SUB, cols), 1)
    sub = lax.broadcasted_iota(jnp.int32, (SUB, cols), 0)
    lane_c = lax.broadcasted_iota(jnp.int32, (CHUNK, cols), 1)
    pair = {w: lane // (2 * w) for w in (1, 2)}

    def geometry(w):
        span = 2 * w * GROUP
        return span, rows // (cols // span)

    def pack(accs, t, k, r0, w):
        span, block = geometry(w)
        accs = list(accs)
        for i in range(CHUNK // SUB):
            r = r0 + SUB * i
            p = span * (r // block) + 2 * w * k
            q = (r % block) // SUB
            turned = pltpu.roll(t[SUB * i:SUB * i + SUB], (p + w) % cols, 1)
            accs[q] = jnp.where(pair[w] == p // (2 * w), turned, accs[q])
        return accs

    def unpack(ed, k, r0, w):
        span, block = geometry(w)
        parts = []
        for i in range(CHUNK // SUB):
            r = r0 + SUB * i
            p = span * (r // block) + 2 * w * k
            q = r % block
            parts.append(pltpu.roll(ed[q:q + SUB], (cols - p) % cols, 1))
        return jnp.concatenate(parts, axis=0)

    def empty(w):
        return [jnp.zeros((SUB, cols), jnp.float32) for _ in range(geometry(w)[1] // SUB)]

    def halo_copies(e, g, w):
        i = e * groups + g
        sx, rx, sp, rp = (
            (xs.at[i], xr.at[i], ps.at[i], pr.at[i]) if w == 1
            else (xs2.at[g], xr2.at[g], ps2.at[g], pr2.at[g])
        )
        plan = (
            (sp, rp.at[0], at(gx, right)),
            (sp, rp.at[1], at(gx, left)),
            (sx.at[0], rx.at[1], at(up, gy)),
            (sx.at[1], rx.at[0], at(down, gy)),
        )
        return [
            pltpu.make_async_remote_copy(
                src_ref=s, dst_ref=r, send_sem=hs_sem.at[e, j // 2], recv_sem=hr_sem.at[i, j // 2],
                device_id=dev, device_id_type=MESH,
            )
            for j, (s, r, dev) in enumerate(plan)
        ]

    def send_halo(e, g, w, accs):
        i = e * groups + g
        ref = ps.at[i] if w == 1 else ps2.at[g]
        for q, v in enumerate(accs):
            ref[SUB * q:SUB * q + SUB, :] = v
        for c in halo_copies(e, g, w):
            c.start()

    def settle(ref, sem):
        pltpu.make_async_copy(ref, ref, sem).wait()

    def take_halo(e, g, w, above, below):
        i = e * groups + g
        rx, rp = (xr.at[i], pr.at[i]) if w == 1 else (xr2.at[g], pr2.at[g])
        settle(rp, hr_sem.at[i, 0])
        settle(rx, hr_sem.at[i, 1])
        for k in range(GROUP):
            for j in range(w):
                m = j * GROUP + k
                above[g * GROUP + k, PAD - w + j:PAD - w + j + 1, :] = rx[0, m:m + 1, :]
                below[g * GROUP + k, PAD + rows + j:PAD + rows + j + 1, :] = rx[1, m:m + 1, :]
        size = geometry(w)[1]
        lanes = lax.broadcasted_iota(jnp.int32, (size, cols), 1)
        return jnp.where(
            lax.rem(lanes, 2 * w) < w, rp[0], pltpu.roll(rp[1], cols - 2 * w, 1)
        )

    def edge_rows(e, g, k, w, first, last):
        i = e * groups + g
        ref = xs.at[i] if w == 1 else xs2.at[g]
        for j in range(w):
            m = j * GROUP + k
            ref[0, m:m + 1, :] = first[j:j + 1]
            ref[1, m:m + 1, :] = last[CHUNK - w + j:CHUNK - w + j + 1]

    def fold(x):
        return jnp.sum(x.reshape(CHUNK // SUB, SUB, cols), axis=0)

    def put(acc, place, part):
        return jnp.where(sub == place, jnp.sum(part, axis=0, keepdims=True), acc)

    def send_sums(s, g, acc):
        i = s * groups + g
        line = jnp.sum(acc, axis=1, keepdims=True)
        row = jnp.sum(jnp.where(lane == sub, line, 0.0), axis=0, keepdims=True)
        ar_out[i] = row
        ar_in[i, me] = row

        def send(dev):
            pltpu.make_async_remote_copy(
                src_ref=ar_out.at[i], dst_ref=ar_in.at[i, me],
                send_sem=as_sem.at[s], recv_sem=ar_sem.at[i],
                device_id=dev, device_id_type=MESH,
            ).start()

        each_peer(send)

    def take_sums(s, g):
        i = s * groups + g
        settle(ar_in.at[i, pl.ds(0, n - 1)], ar_sem.at[i])
        total = jnp.sum(ar_in[i], axis=0)
        line = jnp.sum(jnp.where(lane == sub, total, 0.0), axis=1, keepdims=True)
        return jnp.broadcast_to(line, (SUB, cols))

    def offset_of(g, total):
        return (total - lam_tab[g] * pltpu.roll(total, GROUP, 0)) * (1.0 / cells)

    starts = range(0, rows, CHUNK)
    zero8 = jnp.zeros((SUB, cols), jnp.float32)

    load_d.wait()
    load_c.wait()
    load_k.wait()

    def begin(g, carry):
        def mix(r8, carry):
            r = pl.multiple_of(r8 * SUB, SUB)
            totals = [src[g * GROUP + k, pl.ds(r, SUB), :] for k in range(GROUP)]
            for j in range(classes):
                part = d0[j, pl.ds(PAD + r, SUB), :]
                for k in range(GROUP):
                    totals[k] = totals[k] + coupling[g * GROUP + k, j] * part
            for k in range(GROUP):
                src[g * GROUP + k, pl.ds(r, SUB), :] = totals[k]
            return carry

        lax.fori_loop(0, rows // SUB, mix, 0, unroll=2)
        acc, accs, accs_d = zero8, empty(1), empty(1)
        for k in range(GROUP):
            kk = g * GROUP + k
            total = zero8
            ts, ds = [], []
            for r0 in starts:
                t = src[kk, r0:r0 + CHUNK, :] * 0.5
                dd = d0[kk, PAD + r0:PAD + r0 + CHUNK, :]
                u[kk, PAD + r0:PAD + r0 + CHUNK, :] = t
                accs = pack(accs, t, k, r0, 1)
                accs_d = pack(accs_d, dd, k, r0, 1)
                total = total + fold(t)
                ts.append(t)
                ds.append(dd)
            edge_rows(1, g, k, 1, ts[0], ts[-1])
            edge_rows(0, g, k, 1, ds[0], ds[-1])
            acc = put(acc, k, total)
        lam_tab[g] = zero8

        @pl.when(g == 0)
        def _():
            pl.semaphore_wait(barrier, n - 1)

        send_halo(1, g, 1, accs)
        send_sums(0, g, acc)
        send_halo(0, g, 1, accs_d)
        return carry

    lax.fori_loop(0, groups, begin, 0)

    def neighbours(field, ed, kk, k, r0):
        lo = PAD + r0
        mid = field[kk, lo:lo + CHUNK, :]
        xp = field[kk, lo + 1:lo + 1 + CHUNK, :]
        xm = field[kk, lo - 1:lo - 1 + CHUNK, :]
        side = unpack(ed, k, r0, 1)
        yp = jnp.where(lane_c == cols - 1, side, pltpu.roll(mid, cols - 1, 1))
        ym = jnp.where(lane_c == 0, side, pltpu.roll(mid, 1, 1))
        return xp, xm, yp, ym

    def climb(s, g, w):
        ed = take_halo(s, g, 1, u, u)
        acc = zero8
        for k in range(GROUP):
            kk = g * GROUP + k
            sum_a, sum_b = zero8, zero8
            for r0 in starts:
                xp, xm, yp, ym = neighbours(u, ed, kk, k, r0)
                px = jnp.abs(xp - xm) * 0.5
                py = jnp.abs(yp - ym) * 0.5
                sx, sy = xp + xm, yp + ym
                inv = 1.0 / (2.0 + px + py)
                gain = (sx + sy) + px * (sx - px) + py * (sy - py)
                at_a = (src[kk, r0:r0 + CHUNK, :] + 0.5 * gain) * inv
                a[kk, r0:r0 + CHUNK, :] = at_a
                b[kk, r0:r0 + CHUNK, :] = inv
                sum_a = sum_a + fold(at_a)
                sum_b = sum_b + fold(inv)
            acc = put(put(acc, k, sum_a), GROUP + k, sum_b)
        send_sums(s, g, acc)
        lam_tab[g] = THETA * offset_of(g, take_sums(s - 1, g))
        accs = empty(w)
        for k in range(GROUP):
            kk = g * GROUP + k
            scale = lam_tab[g, k:k + 1, :]
            ts = []
            for r0 in starts:
                t = a[kk, r0:r0 + CHUNK, :] - scale * b[kk, r0:r0 + CHUNK, :]
                u[kk, PAD + r0:PAD + r0 + CHUNK, :] = t
                if w == 2:
                    trial[kk, r0:r0 + CHUNK, :] = t
                accs = pack(accs, t, k, r0, w)
                ts.append(t)
            edge_rows(s + 1, g, k, w, ts[0], ts[-1])
        send_halo(s + 1, g, w, accs)

    def middle(i, carry):
        climb(1 + i // groups, lax.rem(i, groups), 1)
        return carry

    def final(g, carry):
        climb(SWEEPS - 1, g, 2)
        return carry

    lax.fori_loop(0, (SWEEPS - 2) * groups, middle, 0)
    lax.fori_loop(0, groups, final, 0)

    base = SWEEPS + 1
    extra = 2 * SWEEPS

    def weights(g):
        ed2 = take_halo(SWEEPS, g, 2, u, u)
        lanes2 = lax.broadcasted_iota(jnp.int32, ed2.shape, 1)
        ed3 = jnp.where(
            lax.rem(lanes2, 4) < 2, pltpu.roll(ed2, cols - 1, 1), pltpu.roll(ed2, 1, 1)
        )
        for k in range(GROUP):
            kk = g * GROUP + k
            cs = []
            for r0 in starts:
                lo = PAD + r0
                mid = u[kk, lo:lo + CHUNK, :]
                xp = u[kk, lo + 1:lo + 1 + CHUNK, :]
                xm = u[kk, lo - 1:lo - 1 + CHUNK, :]
                xpp = u[kk, lo + 2:lo + 2 + CHUNK, :]
                xmm = u[kk, lo - 2:lo - 2 + CHUNK, :]
                side = unpack(ed2, k, r0, 2)
                near = unpack(ed3, k, r0, 2)
                ypp = jnp.where(lane_c >= cols - 2, side, pltpu.roll(mid, cols - 2, 1))
                ymm = jnp.where(lane_c < 2, side, pltpu.roll(mid, 2, 1))
                yp = jnp.where(lane_c == cols - 1, near, pltpu.roll(mid, cols - 1, 1))
                ym = jnp.where(lane_c == 0, near, pltpu.roll(mid, 1, 1))
                half = 0.5 / (2.0 + 0.5 * (jnp.abs(xp - xm) + jnp.abs(yp - ym)))
                c = [half * (1.0 + jnp.maximum(far - mid, 0.0)) for far in (xpp, xmm, ypp, ymm)]
                cxp[kk, lo:lo + CHUNK, :] = c[0]
                cxm[kk, lo:lo + CHUNK, :] = c[1]
                cyp[kk, r0:r0 + CHUNK, :] = c[2]
                cym[kk, r0:r0 + CHUNK, :] = c[3]
                cs.append(c)
            edge_rows(extra, g, k, 1, cs[0][1], cs[-1][0])

    def send_weights(g):
        accs = empty(1)
        for k in range(GROUP):
            kk = g * GROUP + k
            for r0 in starts:
                rim = jnp.where(lane_c == 0, cym[kk, r0:r0 + CHUNK, :], cyp[kk, r0:r0 + CHUNK, :])
                accs = pack(accs, rim, k, r0, 1)
        send_halo(extra, g, 1, accs)

    def flow(s, g):
        last, counted = s == SWEEPS - 1, s == SWEEPS - 2
        now, then = (d1, d0) if s % 2 else (d0, d1)
        ed = take_halo(base + s - 1 if s else 0, g, 1, now, now)
        accs, acc = empty(1), zero8
        for k in range(GROUP):
            kk = g * GROUP + k
            fs, total = [], zero8
            for r0 in starts:
                lo = PAD + r0
                c = [
                    cxp[kk, lo:lo + CHUNK, :], cxm[kk, lo:lo + CHUNK, :],
                    cyp[kk, r0:r0 + CHUNK, :], cym[kk, r0:r0 + CHUNK, :],
                ]
                xp, xm, yp, ym = neighbours(now, ed, kk, k, r0)
                f = c[0] * xp + c[1] * xm + c[2] * yp + c[3] * ym
                if last:
                    fresh[kk, r0:r0 + CHUNK, :] = f
                    continue
                then[kk, lo:lo + CHUNK, :] = f
                accs = pack(accs, f, k, r0, 1)
                fs.append(f)
                if counted:
                    total = total + fold(f * a[kk, r0:r0 + CHUNK, :])
            if not last:
                edge_rows(base + s, g, k, 1, fs[0], fs[-1])
            if counted:
                acc = put(acc, k, total)
        if not last:
            send_halo(base + s, g, 1, accs)
        if counted:
            send_sums(SWEEPS, g, acc)

    def shares(g):
        ed = take_halo(extra, g, 1, cxp, cxm)
        for k in range(GROUP):
            kk = g * GROUP + k
            for r0 in starts:
                lo = PAD + r0
                side = unpack(ed, k, r0, 1)
                east = pltpu.roll(cym[kk, r0:r0 + CHUNK, :], cols - 1, 1)
                west = pltpu.roll(cyp[kk, r0:r0 + CHUNK, :], 1, 1)
                a[kk, r0:r0 + CHUNK, :] = (
                    (cxp[kk, lo - 1:lo - 1 + CHUNK, :] + cxm[kk, lo + 1:lo + 1 + CHUNK, :])
                    + (jnp.where(lane_c == cols - 1, side, east) + jnp.where(lane_c == 0, side, west))
                )

    def flat(g, line, row):
        mine = (lane == g * GROUP + sub) & (sub < GROUP)
        return row + jnp.sum(jnp.where(mine, line, 0.0), axis=0, keepdims=True)

    def shifts(g, row):
        return flat(g, offset_of(g, take_sums(SWEEPS - 1, g)), row)

    def drain(e):
        part = pl.ds(e * groups, groups)
        rx, rp = (xr2, pr2) if e == SWEEPS else (xr.at[part], pr.at[part])
        settle(rp, hs_sem.at[e, 0])
        settle(rx, hs_sem.at[e, 1])

    def drain_sums(s):
        settle(ar_in.at[pl.ds(s * groups, groups), pl.ds(0, n - 1)], as_sem.at[s])

    end = base + SWEEPS - 2
    for s in range(SWEEPS):

        def flows(g, carry):
            if s == 0:
                weights(g)
            flow(s, g)
            if s == 0:
                send_weights(g)
            if s == SWEEPS - 3:
                shares(g)
            return carry

        if s == SWEEPS - 1:
            means[0:1, :] = lax.fori_loop(0, groups, shifts, jnp.zeros((1, cols), jnp.float32))
            for e in [*range(end), extra]:
                drain(e)
            for j in range(SWEEPS):
                drain_sums(j)
        lax.fori_loop(0, groups, flows, 0)

    drain(end)
    drain_sums(SWEEPS)
    row = jnp.zeros((1, cols), jnp.float32)
    for g in range(groups):
        i = SWEEPS * groups + g
        settle(ar_in.at[i, pl.ds(0, n - 1)], ar_sem.at[i])
        total = jnp.where(lane[0:1] < GROUP, jnp.sum(ar_in[i], axis=0), 0.0)
        row = row + (total if g == 0 else pltpu.roll(total, g * GROUP, 1))
    means[1:2, :] = row * (1.0 / cells)


def shards(cost, density_start, coupling):
    nx, ny = lax.axis_size("gx"), lax.axis_size("gy")
    classes, rows, cols = cost.shape
    f32 = jnp.float32
    n = nx * ny
    groups = classes // GROUP
    full = pltpu.VMEM((classes, rows, cols), f32)
    padded = pltpu.VMEM((classes, rows + 2 * PAD, cols), f32)
    slots = (2 * SWEEPS + 1) * groups
    sums = (SWEEPS + 1) * groups
    block = rows * 2 * GROUP // cols
    trial, fresh, means = pl.pallas_call(
        functools.partial(kernel, nx, ny),
        out_shape=(
            jax.ShapeDtypeStruct(cost.shape, f32),
            jax.ShapeDtypeStruct(cost.shape, f32),
            jax.ShapeDtypeStruct((2, cols), f32),
        ),
        in_specs=[
            pl.BlockSpec(memory_space=pl.ANY),
            pl.BlockSpec(memory_space=pl.ANY),
            pl.BlockSpec(memory_space=pl.ANY),
        ],
        out_specs=(
            pl.BlockSpec(memory_space=pltpu.VMEM),
            pl.BlockSpec(memory_space=pltpu.VMEM),
            pl.BlockSpec(memory_space=pltpu.VMEM),
        ),
        scratch_shapes=[
            pltpu.SMEM(coupling.shape, f32),
            full, padded, full, full,
            padded, padded, padded, padded, full, full,
            pltpu.VMEM((slots, 2, GROUP, cols), f32),
            pltpu.VMEM((slots, 2, GROUP, cols), f32),
            pltpu.VMEM((slots, block, cols), f32),
            pltpu.VMEM((slots, 2, block, cols), f32),
            pltpu.VMEM((groups, 2, 2 * GROUP, cols), f32),
            pltpu.VMEM((groups, 2, 2 * GROUP, cols), f32),
            pltpu.VMEM((groups, 2 * block, cols), f32),
            pltpu.VMEM((groups, 2, 2 * block, cols), f32),
            pltpu.VMEM((sums, 1, cols), f32),
            pltpu.VMEM((sums, n, 1, cols), f32),
            pltpu.VMEM((groups, SUB, cols), f32),
            pltpu.SemaphoreType.DMA((3,)),
            pltpu.SemaphoreType.DMA((2 * SWEEPS + 1, 2)),
            pltpu.SemaphoreType.DMA((slots, 2)),
            pltpu.SemaphoreType.DMA((SWEEPS + 1,)),
            pltpu.SemaphoreType.DMA((sums,)),
        ],
        compiler_params=pltpu.CompilerParams(
            collective_id=0, has_side_effects=True, vmem_limit_bytes=VMEM_LIMIT
        ),
    )(cost, density_start, coupling)
    offset = means[0, :classes]
    mass = means[1, :classes]
    value = trial - offset[:, None, None]
    density = fresh / mass[:, None, None]
    return value, density, THETA * offset


VMEM_LIMIT = 54000000


def solution(mesh):
    placed = P(None, "gx", "gy")
    return jax.shard_map(
        shards,
        mesh=mesh,
        in_specs=(placed, placed, P()),
        out_specs=(placed, placed, P()),
        check_vma=False,
    )
```

```python
import functools

import jax
import jax.numpy as jnp
from jax import lax
from jax.experimental import pallas as pl
from jax.experimental.pallas import tpu as pltpu
from jax.sharding import PartitionSpec as P

MESH = pl.DeviceIdType.MESH
SWEEPS = 5
THETA = 2.0
PAD = 8
CHUNK = 32
SUB = 8
GROUP = 4


def kernel(
    nx, ny,
    cost_hbm, dens_hbm, coup_hbm,
    trial, fresh, means,
    coupling, src, u, a, b, d0, d1, cxp, cxm, cyp, cym,
    xs, xr, ps, pr, xs2, xr2, ps2, pr2,
    ar_out, ar_in, lam_tab,
    in_sem, hs_sem, hr_sem, as_sem, ar_sem,
):
    classes, rows, cols = cost_hbm.shape
    groups = classes // GROUP
    n = nx * ny
    cells = float(n * rows * cols)
    gx, gy = lax.axis_index("gx"), lax.axis_index("gy")
    up, down = lax.rem(gx + nx - 1, nx), lax.rem(gx + 1, nx)
    left, right = lax.rem(gy + ny - 1, ny), lax.rem(gy + 1, ny)
    me = gx * ny + gy

    def at(x, y):
        return {"gx": x, "gy": y}

    def each_peer(body):
        def step(i, carry):
            dx, dy = i // ny, lax.rem(i, ny)
            body(at(lax.rem(gx + dx, nx), lax.rem(gy + dy, ny)))
            return carry

        lax.fori_loop(1, n, step, 0, unroll=n - 1 if n <= 32 else 1)

    load_d = pltpu.make_async_copy(dens_hbm, d0.at[:, pl.ds(PAD, rows), :], in_sem.at[0])
    load_c = pltpu.make_async_copy(cost_hbm, src, in_sem.at[1])
    load_k = pltpu.make_async_copy(coup_hbm, coupling, in_sem.at[2])
    load_d.start()
    load_c.start()
    load_k.start()

    barrier = pltpu.get_barrier_semaphore()
    each_peer(lambda dev: pl.semaphore_signal(barrier, inc=1, device_id=dev, device_id_type=MESH))

    lane = lax.broadcasted_iota(jnp.int32, (SUB, cols), 1)
    sub = lax.broadcasted_iota(jnp.int32, (SUB, cols), 0)
    lane_c = lax.broadcasted_iota(jnp.int32, (CHUNK, cols), 1)
    pair = {w: lane // (2 * w) for w in (1, 2)}

    def geometry(w):
        span = 2 * w * GROUP
        return span, rows // (cols // span)

    def pack(accs, t, k, r0, w):
        span, block = geometry(w)
        accs = list(accs)
        for i in range(CHUNK // SUB):
            r = r0 + SUB * i
            p = span * (r // block) + 2 * w * k
            q = (r % block) // SUB
            turned = pltpu.roll(t[SUB * i:SUB * i + SUB], (p + w) % cols, 1)
            accs[q] = jnp.where(pair[w] == p // (2 * w), turned, accs[q])
        return accs

    def unpack(ed, k, r0, w):
        span, block = geometry(w)
        parts = []
        for i in range(CHUNK // SUB):
            r = r0 + SUB * i
            p = span * (r // block) + 2 * w * k
            q = r % block
            parts.append(pltpu.roll(ed[q:q + SUB], (cols - p) % cols, 1))
        return jnp.concatenate(parts, axis=0)

    def empty(w):
        return [jnp.zeros((SUB, cols), jnp.float32) for _ in range(geometry(w)[1] // SUB)]

    def halo_copies(e, g, w):
        i = e * groups + g
        sx, rx, sp, rp = (
            (xs.at[i], xr.at[i], ps.at[i], pr.at[i]) if w == 1
            else (xs2.at[g], xr2.at[g], ps2.at[g], pr2.at[g])
        )
        plan = (
            (sp, rp.at[0], at(gx, right)),
            (sp, rp.at[1], at(gx, left)),
            (sx.at[0], rx.at[1], at(up, gy)),
            (sx.at[1], rx.at[0], at(down, gy)),
        )
        return [
            pltpu.make_async_remote_copy(
                src_ref=s, dst_ref=r, send_sem=hs_sem.at[e, j // 2], recv_sem=hr_sem.at[i, j // 2],
                device_id=dev, device_id_type=MESH,
            )
            for j, (s, r, dev) in enumerate(plan)
        ]

    def send_halo(e, g, w, accs):
        i = e * groups + g
        ref = ps.at[i] if w == 1 else ps2.at[g]
        for q, v in enumerate(accs):
            ref[SUB * q:SUB * q + SUB, :] = v
        for c in halo_copies(e, g, w):
            c.start()

    def settle(ref, sem):
        pltpu.make_async_copy(ref, ref, sem).wait()

    def take_halo(e, g, w, above, below):
        i = e * groups + g
        rx, rp = (xr.at[i], pr.at[i]) if w == 1 else (xr2.at[g], pr2.at[g])
        settle(rp, hr_sem.at[i, 0])
        settle(rx, hr_sem.at[i, 1])
        for k in range(GROUP):
            for j in range(w):
                m = j * GROUP + k
                above[g * GROUP + k, PAD - w + j:PAD - w + j + 1, :] = rx[0, m:m + 1, :]
                below[g * GROUP + k, PAD + rows + j:PAD + rows + j + 1, :] = rx[1, m:m + 1, :]
        size = geometry(w)[1]
        lanes = lax.broadcasted_iota(jnp.int32, (size, cols), 1)
        return jnp.where(
            lax.rem(lanes, 2 * w) < w, rp[0], pltpu.roll(rp[1], cols - 2 * w, 1)
        )

    def edge_rows(e, g, k, w, first, last):
        i = e * groups + g
        ref = xs.at[i] if w == 1 else xs2.at[g]
        for j in range(w):
            m = j * GROUP + k
            ref[0, m:m + 1, :] = first[j:j + 1]
            ref[1, m:m + 1, :] = last[CHUNK - w + j:CHUNK - w + j + 1]

    def fold(x):
        return jnp.sum(x.reshape(CHUNK // SUB, SUB, cols), axis=0)

    def put(acc, place, part):
        return jnp.where(sub == place, jnp.sum(part, axis=0, keepdims=True), acc)

    def send_sums(s, g, acc):
        i = s * groups + g
        line = jnp.sum(acc, axis=1, keepdims=True)
        row = jnp.sum(jnp.where(lane == sub, line, 0.0), axis=0, keepdims=True)
        ar_out[i] = row
        ar_in[i, me] = row

        def send(dev):
            pltpu.make_async_remote_copy(
                src_ref=ar_out.at[i], dst_ref=ar_in.at[i, me],
                send_sem=as_sem.at[s], recv_sem=ar_sem.at[i],
                device_id=dev, device_id_type=MESH,
            ).start()

        each_peer(send)

    def take_sums(s, g):
        i = s * groups + g
        settle(ar_in.at[i, pl.ds(0, n - 1)], ar_sem.at[i])
        total = jnp.sum(ar_in[i], axis=0)
        line = jnp.sum(jnp.where(lane == sub, total, 0.0), axis=1, keepdims=True)
        return jnp.broadcast_to(line, (SUB, cols))

    def offset_of(g, total):
        return (total - lam_tab[g] * pltpu.roll(total, GROUP, 0)) * (1.0 / cells)

    starts = range(0, rows, CHUNK)
    zero8 = jnp.zeros((SUB, cols), jnp.float32)

    load_d.wait()
    load_c.wait()
    load_k.wait()

    def begin(g, carry):
        def mix(i, carry):
            r = pl.multiple_of(i * CHUNK, CHUNK)
            totals = [src[g * GROUP + k, pl.ds(r, CHUNK), :] for k in range(GROUP)]
            for j in range(classes):
                part = d0[j, pl.ds(PAD + r, CHUNK), :]
                for k in range(GROUP):
                    totals[k] = totals[k] + coupling[g * GROUP + k, j] * part
            for k in range(GROUP):
                src[g * GROUP + k, pl.ds(r, CHUNK), :] = totals[k]
            return carry

        lax.fori_loop(0, rows // CHUNK, mix, 0)
        acc, accs, accs_d = zero8, empty(1), empty(1)
        for k in range(GROUP):
            kk = g * GROUP + k
            total = zero8
            ts, ds = [], []
            for r0 in starts:
                t = src[kk, r0:r0 + CHUNK, :] * 0.5
                dd = d0[kk, PAD + r0:PAD + r0 + CHUNK, :]
                u[kk, PAD + r0:PAD + r0 + CHUNK, :] = t
                accs = pack(accs, t, k, r0, 1)
                accs_d = pack(accs_d, dd, k, r0, 1)
                total = total + fold(t)
                ts.append(t)
                ds.append(dd)
            edge_rows(1, g, k, 1, ts[0], ts[-1])
            edge_rows(0, g, k, 1, ds[0], ds[-1])
            acc = put(acc, k, total)
        lam_tab[g] = zero8

        @pl.when(g == 0)
        def _():
            pl.semaphore_wait(barrier, n - 1)

        send_halo(1, g, 1, accs)
        send_sums(0, g, acc)
        send_halo(0, g, 1, accs_d)
        return carry

    lax.fori_loop(0, groups, begin, 0)

    def neighbours(field, ed, kk, k, r0):
        lo = PAD + r0
        mid = field[kk, lo:lo + CHUNK, :]
        xp = field[kk, lo + 1:lo + 1 + CHUNK, :]
        xm = field[kk, lo - 1:lo - 1 + CHUNK, :]
        side = unpack(ed, k, r0, 1)
        yp = jnp.where(lane_c == cols - 1, side, pltpu.roll(mid, cols - 1, 1))
        ym = jnp.where(lane_c == 0, side, pltpu.roll(mid, 1, 1))
        return xp, xm, yp, ym

    def climb(s, g, w):
        ed = take_halo(s, g, 1, u, u)
        acc = zero8
        for k in range(GROUP):
            kk = g * GROUP + k
            sum_a, sum_b = zero8, zero8
            for r0 in starts:
                xp, xm, yp, ym = neighbours(u, ed, kk, k, r0)
                px = jnp.abs(xp - xm) * 0.5
                py = jnp.abs(yp - ym) * 0.5
                sx, sy = xp + xm, yp + ym
                inv = 1.0 / (2.0 + px + py)
                gain = (sx + sy) + px * (sx - px) + py * (sy - py)
                at_a = (src[kk, r0:r0 + CHUNK, :] + 0.5 * gain) * inv
                a[kk, r0:r0 + CHUNK, :] = at_a
                b[kk, r0:r0 + CHUNK, :] = inv
                sum_a = sum_a + fold(at_a)
                sum_b = sum_b + fold(inv)
            acc = put(put(acc, k, sum_a), GROUP + k, sum_b)
        send_sums(s, g, acc)
        lam_tab[g] = THETA * offset_of(g, take_sums(s - 1, g))
        accs = empty(w)
        for k in range(GROUP):
            kk = g * GROUP + k
            scale = lam_tab[g, k:k + 1, :]
            ts = []
            for r0 in starts:
                t = a[kk, r0:r0 + CHUNK, :] - scale * b[kk, r0:r0 + CHUNK, :]
                u[kk, PAD + r0:PAD + r0 + CHUNK, :] = t
                if w == 2:
                    trial[kk, r0:r0 + CHUNK, :] = t
                accs = pack(accs, t, k, r0, w)
                ts.append(t)
            edge_rows(s + 1, g, k, w, ts[0], ts[-1])
        send_halo(s + 1, g, w, accs)

    def middle(i, carry):
        climb(1 + i // groups, lax.rem(i, groups), 1)
        return carry

    def final(g, carry):
        climb(SWEEPS - 1, g, 2)
        return carry

    lax.fori_loop(0, (SWEEPS - 2) * groups, middle, 0)
    lax.fori_loop(0, groups, final, 0)

    base = SWEEPS + 1
    extra = 2 * SWEEPS

    def weights(g):
        ed2 = take_halo(SWEEPS, g, 2, u, u)
        lanes2 = lax.broadcasted_iota(jnp.int32, ed2.shape, 1)
        ed3 = jnp.where(
            lax.rem(lanes2, 4) < 2, pltpu.roll(ed2, cols - 1, 1), pltpu.roll(ed2, 1, 1)
        )
        for k in range(GROUP):
            kk = g * GROUP + k
            cs = []
            for r0 in starts:
                lo = PAD + r0
                mid = u[kk, lo:lo + CHUNK, :]
                xp = u[kk, lo + 1:lo + 1 + CHUNK, :]
                xm = u[kk, lo - 1:lo - 1 + CHUNK, :]
                xpp = u[kk, lo + 2:lo + 2 + CHUNK, :]
                xmm = u[kk, lo - 2:lo - 2 + CHUNK, :]
                side = unpack(ed2, k, r0, 2)
                near = unpack(ed3, k, r0, 2)
                ypp = jnp.where(lane_c >= cols - 2, side, pltpu.roll(mid, cols - 2, 1))
                ymm = jnp.where(lane_c < 2, side, pltpu.roll(mid, 2, 1))
                yp = jnp.where(lane_c == cols - 1, near, pltpu.roll(mid, cols - 1, 1))
                ym = jnp.where(lane_c == 0, near, pltpu.roll(mid, 1, 1))
                half = 0.5 / (2.0 + 0.5 * (jnp.abs(xp - xm) + jnp.abs(yp - ym)))
                c = [half * (1.0 + jnp.maximum(far - mid, 0.0)) for far in (xpp, xmm, ypp, ymm)]
                cxp[kk, lo:lo + CHUNK, :] = c[0]
                cxm[kk, lo:lo + CHUNK, :] = c[1]
                cyp[kk, r0:r0 + CHUNK, :] = c[2]
                cym[kk, r0:r0 + CHUNK, :] = c[3]
                cs.append(c)
            edge_rows(extra, g, k, 1, cs[0][1], cs[-1][0])

    def send_weights(g):
        accs = empty(1)
        for k in range(GROUP):
            kk = g * GROUP + k
            for r0 in starts:
                rim = jnp.where(lane_c == 0, cym[kk, r0:r0 + CHUNK, :], cyp[kk, r0:r0 + CHUNK, :])
                accs = pack(accs, rim, k, r0, 1)
        send_halo(extra, g, 1, accs)

    def flow(s, g):
        last, counted = s == SWEEPS - 1, s == SWEEPS - 2
        now, then = (d1, d0) if s % 2 else (d0, d1)
        ed = take_halo(base + s - 1 if s else 0, g, 1, now, now)
        accs, acc = empty(1), zero8
        for k in range(GROUP):
            kk = g * GROUP + k
            fs, total = [], zero8
            for r0 in starts:
                lo = PAD + r0
                c = [
                    cxp[kk, lo:lo + CHUNK, :], cxm[kk, lo:lo + CHUNK, :],
                    cyp[kk, r0:r0 + CHUNK, :], cym[kk, r0:r0 + CHUNK, :],
                ]
                xp, xm, yp, ym = neighbours(now, ed, kk, k, r0)
                f = c[0] * xp + c[1] * xm + c[2] * yp + c[3] * ym
                if last:
                    fresh[kk, r0:r0 + CHUNK, :] = f
                    continue
                then[kk, lo:lo + CHUNK, :] = f
                accs = pack(accs, f, k, r0, 1)
                fs.append(f)
                if counted:
                    total = total + fold(f * a[kk, r0:r0 + CHUNK, :])
            if not last:
                edge_rows(base + s, g, k, 1, fs[0], fs[-1])
            if counted:
                acc = put(acc, k, total)
        if not last:
            send_halo(base + s, g, 1, accs)
        if counted:
            send_sums(SWEEPS, g, acc)

    def shares(g):
        ed = take_halo(extra, g, 1, cxp, cxm)
        for k in range(GROUP):
            kk = g * GROUP + k
            for r0 in starts:
                lo = PAD + r0
                side = unpack(ed, k, r0, 1)
                east = pltpu.roll(cym[kk, r0:r0 + CHUNK, :], cols - 1, 1)
                west = pltpu.roll(cyp[kk, r0:r0 + CHUNK, :], 1, 1)
                a[kk, r0:r0 + CHUNK, :] = (
                    (cxp[kk, lo - 1:lo - 1 + CHUNK, :] + cxm[kk, lo + 1:lo + 1 + CHUNK, :])
                    + (jnp.where(lane_c == cols - 1, side, east) + jnp.where(lane_c == 0, side, west))
                )

    def flat(g, line, row):
        mine = (lane == g * GROUP + sub) & (sub < GROUP)
        return row + jnp.sum(jnp.where(mine, line, 0.0), axis=0, keepdims=True)

    def shifts(g, row):
        return flat(g, offset_of(g, take_sums(SWEEPS - 1, g)), row)

    def drain(e):
        part = pl.ds(e * groups, groups)
        rx, rp = (xr2, pr2) if e == SWEEPS else (xr.at[part], pr.at[part])
        settle(rp, hs_sem.at[e, 0])
        settle(rx, hs_sem.at[e, 1])

    def drain_sums(s):
        settle(ar_in.at[pl.ds(s * groups, groups), pl.ds(0, n - 1)], as_sem.at[s])

    end = base + SWEEPS - 2
    for s in range(SWEEPS):

        def flows(g, carry):
            if s == 0:
                weights(g)
            flow(s, g)
            if s == 1:
                send_weights(g)
            if s == SWEEPS - 3:
                shares(g)
            return carry

        if s == SWEEPS - 1:
            means[0:1, :] = lax.fori_loop(0, groups, shifts, jnp.zeros((1, cols), jnp.float32))
            for e in [*range(end), extra]:
                drain(e)
            for j in range(SWEEPS):
                drain_sums(j)
        lax.fori_loop(0, groups, flows, 0)

    drain(end)
    drain_sums(SWEEPS)
    row = jnp.zeros((1, cols), jnp.float32)
    for g in range(groups):
        i = SWEEPS * groups + g
        settle(ar_in.at[i, pl.ds(0, n - 1)], ar_sem.at[i])
        total = jnp.where(lane[0:1] < GROUP, jnp.sum(ar_in[i], axis=0), 0.0)
        row = row + (total if g == 0 else pltpu.roll(total, g * GROUP, 1))
    means[1:2, :] = row * (1.0 / cells)


def shards(cost, density_start, coupling):
    nx, ny = lax.axis_size("gx"), lax.axis_size("gy")
    classes, rows, cols = cost.shape
    f32 = jnp.float32
    n = nx * ny
    groups = classes // GROUP
    full = pltpu.VMEM((classes, rows, cols), f32)
    padded = pltpu.VMEM((classes, rows + 2 * PAD, cols), f32)
    slots = (2 * SWEEPS + 1) * groups
    sums = (SWEEPS + 1) * groups
    block = rows * 2 * GROUP // cols
    trial, fresh, means = pl.pallas_call(
        functools.partial(kernel, nx, ny),
        out_shape=(
            jax.ShapeDtypeStruct(cost.shape, f32),
            jax.ShapeDtypeStruct(cost.shape, f32),
            jax.ShapeDtypeStruct((2, cols), f32),
        ),
        in_specs=[
            pl.BlockSpec(memory_space=pl.ANY),
            pl.BlockSpec(memory_space=pl.ANY),
            pl.BlockSpec(memory_space=pl.ANY),
        ],
        out_specs=(
            pl.BlockSpec(memory_space=pltpu.VMEM),
            pl.BlockSpec(memory_space=pltpu.VMEM),
            pl.BlockSpec(memory_space=pltpu.VMEM),
        ),
        scratch_shapes=[
            pltpu.SMEM(coupling.shape, f32),
            full, padded, full, full,
            padded, padded, padded, padded, full, full,
            pltpu.VMEM((slots, 2, GROUP, cols), f32),
            pltpu.VMEM((slots, 2, GROUP, cols), f32),
            pltpu.VMEM((slots, block, cols), f32),
            pltpu.VMEM((slots, 2, block, cols), f32),
            pltpu.VMEM((groups, 2, 2 * GROUP, cols), f32),
            pltpu.VMEM((groups, 2, 2 * GROUP, cols), f32),
            pltpu.VMEM((groups, 2 * block, cols), f32),
            pltpu.VMEM((groups, 2, 2 * block, cols), f32),
            pltpu.VMEM((sums, 1, cols), f32),
            pltpu.VMEM((sums, n, 1, cols), f32),
            pltpu.VMEM((groups, SUB, cols), f32),
            pltpu.SemaphoreType.DMA((3,)),
            pltpu.SemaphoreType.DMA((2 * SWEEPS + 1, 2)),
            pltpu.SemaphoreType.DMA((slots, 2)),
            pltpu.SemaphoreType.DMA((SWEEPS + 1,)),
            pltpu.SemaphoreType.DMA((sums,)),
        ],
        compiler_params=pltpu.CompilerParams(
            collective_id=0, has_side_effects=True, vmem_limit_bytes=VMEM_LIMIT
        ),
    )(cost, density_start, coupling)
    offset = means[0, :classes]
    mass = means[1, :classes]
    value = trial - offset[:, None, None]
    density = fresh / mass[:, None, None]
    return value, density, THETA * offset


VMEM_LIMIT = 54000000


def solution(mesh):
    placed = P(None, "gx", "gy")
    return jax.shard_map(
        shards,
        mesh=mesh,
        in_specs=(placed, placed, P()),
        out_specs=(placed, placed, P()),
        check_vma=False,
    )
```

```python
import functools

import jax
import jax.numpy as jnp
from jax import lax
from jax.experimental import pallas as pl
from jax.experimental.pallas import tpu as pltpu
from jax.sharding import PartitionSpec as P

MESH = pl.DeviceIdType.MESH
SWEEPS = 5
THETA = 2.0
PAD = 8
CHUNK = 32
SUB = 8
GROUP = 4


def kernel(
    nx, ny,
    cost_hbm, dens_hbm, coup_hbm,
    trial, fresh, means,
    coupling, src, u, a, b, d0, d1, cxp, cxm, cyp, cym,
    xs, xr, ps, pr, xs2, xr2, ps2, pr2,
    ar_out, ar_in, lam_tab,
    in_sem, hs_sem, hr_sem, as_sem, ar_sem,
):
    classes, rows, cols = cost_hbm.shape
    groups = classes // GROUP
    n = nx * ny
    cells = float(n * rows * cols)
    gx, gy = lax.axis_index("gx"), lax.axis_index("gy")
    up, down = lax.rem(gx + nx - 1, nx), lax.rem(gx + 1, nx)
    left, right = lax.rem(gy + ny - 1, ny), lax.rem(gy + 1, ny)
    me = gx * ny + gy

    def at(x, y):
        return {"gx": x, "gy": y}

    def each_peer(body):
        def step(i, carry):
            dx, dy = i // ny, lax.rem(i, ny)
            body(at(lax.rem(gx + dx, nx), lax.rem(gy + dy, ny)))
            return carry

        if n > 32:
            lax.fori_loop(1, n, step, 0)
            return
        for i in sorted(range(1, n), key=lambda i: -min(i // ny, nx - i // ny)):
            step(i, 0)

    load_d = pltpu.make_async_copy(dens_hbm, d0.at[:, pl.ds(PAD, rows), :], in_sem.at[0])
    load_c = pltpu.make_async_copy(cost_hbm, src, in_sem.at[1])
    load_k = pltpu.make_async_copy(coup_hbm, coupling, in_sem.at[2])
    load_d.start()
    load_c.start()
    load_k.start()

    barrier = pltpu.get_barrier_semaphore()
    each_peer(lambda dev: pl.semaphore_signal(barrier, inc=1, device_id=dev, device_id_type=MESH))

    lane = lax.broadcasted_iota(jnp.int32, (SUB, cols), 1)
    sub = lax.broadcasted_iota(jnp.int32, (SUB, cols), 0)
    lane_c = lax.broadcasted_iota(jnp.int32, (CHUNK, cols), 1)
    pair = {w: lane // (2 * w) for w in (1, 2)}

    def geometry(w):
        span = 2 * w * GROUP
        return span, rows // (cols // span)

    def pack(accs, t, k, r0, w):
        span, block = geometry(w)
        accs = list(accs)
        for i in range(CHUNK // SUB):
            r = r0 + SUB * i
            p = span * (r // block) + 2 * w * k
            q = (r % block) // SUB
            turned = pltpu.roll(t[SUB * i:SUB * i + SUB], (p + w) % cols, 1)
            accs[q] = jnp.where(pair[w] == p // (2 * w), turned, accs[q])
        return accs

    def unpack(ed, k, r0, w):
        span, block = geometry(w)
        parts = []
        for i in range(CHUNK // SUB):
            r = r0 + SUB * i
            p = span * (r // block) + 2 * w * k
            q = r % block
            parts.append(pltpu.roll(ed[q:q + SUB], (cols - p) % cols, 1))
        return jnp.concatenate(parts, axis=0)

    def empty(w):
        return [jnp.zeros((SUB, cols), jnp.float32) for _ in range(geometry(w)[1] // SUB)]

    def halo_copies(e, g, w):
        i = e * groups + g
        sx, rx, sp, rp = (
            (xs.at[i], xr.at[i], ps.at[i], pr.at[i]) if w == 1
            else (xs2.at[g], xr2.at[g], ps2.at[g], pr2.at[g])
        )
        plan = (
            (sp, rp.at[0], at(gx, right)),
            (sp, rp.at[1], at(gx, left)),
            (sx.at[0], rx.at[1], at(up, gy)),
            (sx.at[1], rx.at[0], at(down, gy)),
        )
        return [
            pltpu.make_async_remote_copy(
                src_ref=s, dst_ref=r, send_sem=hs_sem.at[e, j // 2], recv_sem=hr_sem.at[i, j // 2],
                device_id=dev, device_id_type=MESH,
            )
            for j, (s, r, dev) in enumerate(plan)
        ]

    def send_halo(e, g, w, accs):
        i = e * groups + g
        ref = ps.at[i] if w == 1 else ps2.at[g]
        for q, v in enumerate(accs):
            ref[SUB * q:SUB * q + SUB, :] = v
        for c in halo_copies(e, g, w):
            c.start()

    def settle(ref, sem):
        pltpu.make_async_copy(ref, ref, sem).wait()

    def take_halo(e, g, w, above, below):
        i = e * groups + g
        rx, rp = (xr.at[i], pr.at[i]) if w == 1 else (xr2.at[g], pr2.at[g])
        settle(rp, hr_sem.at[i, 0])
        settle(rx, hr_sem.at[i, 1])
        for k in range(GROUP):
            for j in range(w):
                m = j * GROUP + k
                above[g * GROUP + k, PAD - w + j:PAD - w + j + 1, :] = rx[0, m:m + 1, :]
                below[g * GROUP + k, PAD + rows + j:PAD + rows + j + 1, :] = rx[1, m:m + 1, :]
        size = geometry(w)[1]
        lanes = lax.broadcasted_iota(jnp.int32, (size, cols), 1)
        return jnp.where(
            lax.rem(lanes, 2 * w) < w, rp[0], pltpu.roll(rp[1], cols - 2 * w, 1)
        )

    def edge_rows(e, g, k, w, first, last):
        i = e * groups + g
        ref = xs.at[i] if w == 1 else xs2.at[g]
        for j in range(w):
            m = j * GROUP + k
            ref[0, m:m + 1, :] = first[j:j + 1]
            ref[1, m:m + 1, :] = last[CHUNK - w + j:CHUNK - w + j + 1]

    def fold(x):
        return jnp.sum(x.reshape(CHUNK // SUB, SUB, cols), axis=0)

    def put(acc, place, part):
        return jnp.where(sub == place, jnp.sum(part, axis=0, keepdims=True), acc)

    def send_sums(s, g, acc):
        i = s * groups + g
        line = jnp.sum(acc, axis=1, keepdims=True)
        row = jnp.sum(jnp.where(lane == sub, line, 0.0), axis=0, keepdims=True)
        ar_out[i] = row
        ar_in[i, me] = row

        def send(dev):
            pltpu.make_async_remote_copy(
                src_ref=ar_out.at[i], dst_ref=ar_in.at[i, me],
                send_sem=as_sem.at[s], recv_sem=ar_sem.at[i],
                device_id=dev, device_id_type=MESH,
            ).start()

        each_peer(send)

    def take_sums(s, g):
        i = s * groups + g
        settle(ar_in.at[i, pl.ds(0, n - 1)], ar_sem.at[i])
        total = jnp.sum(ar_in[i], axis=0)
        line = jnp.sum(jnp.where(lane == sub, total, 0.0), axis=1, keepdims=True)
        return jnp.broadcast_to(line, (SUB, cols))

    def offset_of(g, total):
        return (total - lam_tab[g] * pltpu.roll(total, GROUP, 0)) * (1.0 / cells)

    starts = range(0, rows, CHUNK)
    zero8 = jnp.zeros((SUB, cols), jnp.float32)

    load_d.wait()
    load_c.wait()
    load_k.wait()

    def begin(g, carry):
        def mix(i, carry):
            r = pl.multiple_of(i * CHUNK, CHUNK)
            totals = [src[g * GROUP + k, pl.ds(r, CHUNK), :] for k in range(GROUP)]
            for j in range(classes):
                part = d0[j, pl.ds(PAD + r, CHUNK), :]
                for k in range(GROUP):
                    totals[k] = totals[k] + coupling[g * GROUP + k, j] * part
            for k in range(GROUP):
                src[g * GROUP + k, pl.ds(r, CHUNK), :] = totals[k]
            return carry

        lax.fori_loop(0, rows // CHUNK, mix, 0)
        acc, accs, accs_d = zero8, empty(1), empty(1)
        for k in range(GROUP):
            kk = g * GROUP + k
            total = zero8
            ts, ds = [], []
            for r0 in starts:
                t = src[kk, r0:r0 + CHUNK, :] * 0.5
                dd = d0[kk, PAD + r0:PAD + r0 + CHUNK, :]
                u[kk, PAD + r0:PAD + r0 + CHUNK, :] = t
                accs = pack(accs, t, k, r0, 1)
                accs_d = pack(accs_d, dd, k, r0, 1)
                total = total + fold(t)
                ts.append(t)
                ds.append(dd)
            edge_rows(1, g, k, 1, ts[0], ts[-1])
            edge_rows(0, g, k, 1, ds[0], ds[-1])
            acc = put(acc, k, total)
        lam_tab[g] = zero8

        @pl.when(g == 0)
        def _():
            pl.semaphore_wait(barrier, n - 1)

        send_sums(0, g, acc)
        send_halo(1, g, 1, accs)
        send_halo(0, g, 1, accs_d)
        return carry

    lax.fori_loop(0, groups, begin, 0)

    def neighbours(field, ed, kk, k, r0):
        lo = PAD + r0
        mid = field[kk, lo:lo + CHUNK, :]
        xp = field[kk, lo + 1:lo + 1 + CHUNK, :]
        xm = field[kk, lo - 1:lo - 1 + CHUNK, :]
        side = unpack(ed, k, r0, 1)
        yp = jnp.where(lane_c == cols - 1, side, pltpu.roll(mid, cols - 1, 1))
        ym = jnp.where(lane_c == 0, side, pltpu.roll(mid, 1, 1))
        return xp, xm, yp, ym

    def climb(s, g, w):
        ed = take_halo(s, g, 1, u, u)
        acc = zero8
        for k in range(GROUP):
            kk = g * GROUP + k
            sum_a, sum_b = zero8, zero8
            for r0 in starts:
                xp, xm, yp, ym = neighbours(u, ed, kk, k, r0)
                px = jnp.abs(xp - xm) * 0.5
                py = jnp.abs(yp - ym) * 0.5
                sx, sy = xp + xm, yp + ym
                inv = 1.0 / (2.0 + px + py)
                gain = (sx + sy) + px * (sx - px) + py * (sy - py)
                at_a = (src[kk, r0:r0 + CHUNK, :] + 0.5 * gain) * inv
                a[kk, r0:r0 + CHUNK, :] = at_a
                b[kk, r0:r0 + CHUNK, :] = inv
                sum_a = sum_a + fold(at_a)
                sum_b = sum_b + fold(inv)
            acc = put(put(acc, k, sum_a), GROUP + k, sum_b)
        send_sums(s, g, acc)
        lam_tab[g] = THETA * offset_of(g, take_sums(s - 1, g))
        accs = empty(w)
        for k in range(GROUP):
            kk = g * GROUP + k
            scale = lam_tab[g, k:k + 1, :]
            ts = []
            for r0 in starts:
                t = a[kk, r0:r0 + CHUNK, :] - scale * b[kk, r0:r0 + CHUNK, :]
                u[kk, PAD + r0:PAD + r0 + CHUNK, :] = t
                if w == 2:
                    trial[kk, r0:r0 + CHUNK, :] = t
                accs = pack(accs, t, k, r0, w)
                ts.append(t)
            edge_rows(s + 1, g, k, w, ts[0], ts[-1])
        send_halo(s + 1, g, w, accs)

    def middle(i, carry):
        climb(1 + i // groups, lax.rem(i, groups), 1)
        return carry

    def final(g, carry):
        climb(SWEEPS - 1, g, 2)
        return carry

    lax.fori_loop(0, (SWEEPS - 2) * groups, middle, 0)
    lax.fori_loop(0, groups, final, 0)

    base = SWEEPS + 1
    extra = 2 * SWEEPS

    def weights(g):
        ed2 = take_halo(SWEEPS, g, 2, u, u)
        lanes2 = lax.broadcasted_iota(jnp.int32, ed2.shape, 1)
        ed3 = jnp.where(
            lax.rem(lanes2, 4) < 2, pltpu.roll(ed2, cols - 1, 1), pltpu.roll(ed2, 1, 1)
        )
        for k in range(GROUP):
            kk = g * GROUP + k
            cs = []
            for r0 in starts:
                lo = PAD + r0
                mid = u[kk, lo:lo + CHUNK, :]
                xp = u[kk, lo + 1:lo + 1 + CHUNK, :]
                xm = u[kk, lo - 1:lo - 1 + CHUNK, :]
                xpp = u[kk, lo + 2:lo + 2 + CHUNK, :]
                xmm = u[kk, lo - 2:lo - 2 + CHUNK, :]
                side = unpack(ed2, k, r0, 2)
                near = unpack(ed3, k, r0, 2)
                ypp = jnp.where(lane_c >= cols - 2, side, pltpu.roll(mid, cols - 2, 1))
                ymm = jnp.where(lane_c < 2, side, pltpu.roll(mid, 2, 1))
                yp = jnp.where(lane_c == cols - 1, near, pltpu.roll(mid, cols - 1, 1))
                ym = jnp.where(lane_c == 0, near, pltpu.roll(mid, 1, 1))
                half = 0.5 / (2.0 + 0.5 * (jnp.abs(xp - xm) + jnp.abs(yp - ym)))
                c = [half * (1.0 + jnp.maximum(far - mid, 0.0)) for far in (xpp, xmm, ypp, ymm)]
                cxp[kk, lo:lo + CHUNK, :] = c[0]
                cxm[kk, lo:lo + CHUNK, :] = c[1]
                cyp[kk, r0:r0 + CHUNK, :] = c[2]
                cym[kk, r0:r0 + CHUNK, :] = c[3]
                cs.append(c)
            edge_rows(extra, g, k, 1, cs[0][1], cs[-1][0])

    def send_weights(g):
        accs = empty(1)
        for k in range(GROUP):
            kk = g * GROUP + k
            for r0 in starts:
                rim = jnp.where(lane_c == 0, cym[kk, r0:r0 + CHUNK, :], cyp[kk, r0:r0 + CHUNK, :])
                accs = pack(accs, rim, k, r0, 1)
        send_halo(extra, g, 1, accs)

    def flow(s, g):
        last, counted = s == SWEEPS - 1, s == SWEEPS - 2
        now, then = (d1, d0) if s % 2 else (d0, d1)
        ed = take_halo(base + s - 1 if s else 0, g, 1, now, now)
        accs, acc = empty(1), zero8
        for k in range(GROUP):
            kk = g * GROUP + k
            fs, total = [], zero8
            for r0 in starts:
                lo = PAD + r0
                c = [
                    cxp[kk, lo:lo + CHUNK, :], cxm[kk, lo:lo + CHUNK, :],
                    cyp[kk, r0:r0 + CHUNK, :], cym[kk, r0:r0 + CHUNK, :],
                ]
                xp, xm, yp, ym = neighbours(now, ed, kk, k, r0)
                f = c[0] * xp + c[1] * xm + c[2] * yp + c[3] * ym
                if last:
                    fresh[kk, r0:r0 + CHUNK, :] = f
                    continue
                then[kk, lo:lo + CHUNK, :] = f
                accs = pack(accs, f, k, r0, 1)
                fs.append(f)
                if counted:
                    total = total + fold(f * a[kk, r0:r0 + CHUNK, :])
            if not last:
                edge_rows(base + s, g, k, 1, fs[0], fs[-1])
            if counted:
                acc = put(acc, k, total)
        if not last:
            send_halo(base + s, g, 1, accs)
        if counted:
            send_sums(SWEEPS, g, acc)

    def shares(g):
        ed = take_halo(extra, g, 1, cxp, cxm)
        for k in range(GROUP):
            kk = g * GROUP + k
            for r0 in starts:
                lo = PAD + r0
                side = unpack(ed, k, r0, 1)
                east = pltpu.roll(cym[kk, r0:r0 + CHUNK, :], cols - 1, 1)
                west = pltpu.roll(cyp[kk, r0:r0 + CHUNK, :], 1, 1)
                a[kk, r0:r0 + CHUNK, :] = (
                    (cxp[kk, lo - 1:lo - 1 + CHUNK, :] + cxm[kk, lo + 1:lo + 1 + CHUNK, :])
                    + (jnp.where(lane_c == cols - 1, side, east) + jnp.where(lane_c == 0, side, west))
                )

    def flat(g, line, row):
        mine = (lane == g * GROUP + sub) & (sub < GROUP)
        return row + jnp.sum(jnp.where(mine, line, 0.0), axis=0, keepdims=True)

    def shifts(g, row):
        return flat(g, offset_of(g, take_sums(SWEEPS - 1, g)), row)

    def drain(e):
        part = pl.ds(e * groups, groups)
        rx, rp = (xr2, pr2) if e == SWEEPS else (xr.at[part], pr.at[part])
        settle(rp, hs_sem.at[e, 0])
        settle(rx, hs_sem.at[e, 1])

    def drain_sums(s):
        settle(ar_in.at[pl.ds(s * groups, groups), pl.ds(0, n - 1)], as_sem.at[s])

    end = base + SWEEPS - 2
    for s in range(SWEEPS):

        def flows(g, carry):
            if s == 0:
                weights(g)
            flow(s, g)
            if s == 1:
                send_weights(g)
            if s == SWEEPS - 3:
                shares(g)
            return carry

        if s == SWEEPS - 1:
            means[0:1, :] = lax.fori_loop(0, groups, shifts, jnp.zeros((1, cols), jnp.float32))
            for e in [*range(end), extra]:
                drain(e)
            for j in range(SWEEPS):
                drain_sums(j)
        lax.fori_loop(0, groups, flows, 0)

    drain(end)
    drain_sums(SWEEPS)
    row = jnp.zeros((1, cols), jnp.float32)
    for g in range(groups):
        i = SWEEPS * groups + g
        settle(ar_in.at[i, pl.ds(0, n - 1)], ar_sem.at[i])
        total = jnp.where(lane[0:1] < GROUP, jnp.sum(ar_in[i], axis=0), 0.0)
        row = row + (total if g == 0 else pltpu.roll(total, g * GROUP, 1))
    means[1:2, :] = row * (1.0 / cells)


def shards(cost, density_start, coupling):
    nx, ny = lax.axis_size("gx"), lax.axis_size("gy")
    classes, rows, cols = cost.shape
    f32 = jnp.float32
    n = nx * ny
    groups = classes // GROUP
    full = pltpu.VMEM((classes, rows, cols), f32)
    padded = pltpu.VMEM((classes, rows + 2 * PAD, cols), f32)
    slots = (2 * SWEEPS + 1) * groups
    sums = (SWEEPS + 1) * groups
    block = rows * 2 * GROUP // cols
    trial, fresh, means = pl.pallas_call(
        functools.partial(kernel, nx, ny),
        out_shape=(
            jax.ShapeDtypeStruct(cost.shape, f32),
            jax.ShapeDtypeStruct(cost.shape, f32),
            jax.ShapeDtypeStruct((2, cols), f32),
        ),
        in_specs=[
            pl.BlockSpec(memory_space=pl.ANY),
            pl.BlockSpec(memory_space=pl.ANY),
            pl.BlockSpec(memory_space=pl.ANY),
        ],
        out_specs=(
            pl.BlockSpec(memory_space=pltpu.VMEM),
            pl.BlockSpec(memory_space=pltpu.VMEM),
            pl.BlockSpec(memory_space=pltpu.VMEM),
        ),
        scratch_shapes=[
            pltpu.SMEM(coupling.shape, f32),
            full, padded, full, full,
            padded, padded, padded, padded, full, full,
            pltpu.VMEM((slots, 2, GROUP, cols), f32),
            pltpu.VMEM((slots, 2, GROUP, cols), f32),
            pltpu.VMEM((slots, block, cols), f32),
            pltpu.VMEM((slots, 2, block, cols), f32),
            pltpu.VMEM((groups, 2, 2 * GROUP, cols), f32),
            pltpu.VMEM((groups, 2, 2 * GROUP, cols), f32),
            pltpu.VMEM((groups, 2 * block, cols), f32),
            pltpu.VMEM((groups, 2, 2 * block, cols), f32),
            pltpu.VMEM((sums, 1, cols), f32),
            pltpu.VMEM((sums, n, 1, cols), f32),
            pltpu.VMEM((groups, SUB, cols), f32),
            pltpu.SemaphoreType.DMA((3,)),
            pltpu.SemaphoreType.DMA((2 * SWEEPS + 1, 2)),
            pltpu.SemaphoreType.DMA((slots, 2)),
            pltpu.SemaphoreType.DMA((SWEEPS + 1,)),
            pltpu.SemaphoreType.DMA((sums,)),
        ],
        compiler_params=pltpu.CompilerParams(
            collective_id=0, has_side_effects=True, vmem_limit_bytes=VMEM_LIMIT
        ),
    )(cost, density_start, coupling)
    offset = means[0, :classes]
    mass = means[1, :classes]
    value = trial - offset[:, None, None]
    density = fresh / mass[:, None, None]
    return value, density, THETA * offset


VMEM_LIMIT = 54000000


def solution(mesh):
    placed = P(None, "gx", "gy")
    return jax.shard_map(
        shards,
        mesh=mesh,
        in_specs=(placed, placed, P()),
        out_specs=(placed, placed, P()),
        check_vma=False,
    )
```
